512 devices in a mesh: seq: 64 (over z_hi, x, y), head: 8 (over z_lo, core).
Axes of the slice: x: 4, y: 8, z: 8 (z_hi: 2, z_lo: 4; z = z_hi * 4 + z_lo), core: 2. Of those that a mesh axis runs over, the one named last changes fastest.
Arguments:
- queries: bfloat16 [12288, 32, 128], P('seq', 'head'), may hold values from -180 to 180
- key_rows: bfloat16 [12288, 8, 128], P('seq', 'head'), may hold values from -4.5 to 4.5
- value_rows: bfloat16 [12288, 8, 128], P('seq', 'head'), may hold values from -24 to 24
- windows: int32 [32], P('head'), may hold values from 768 to 1536, as said below
- sink_counts: int32 [32], P('head'), may hold values from 1 to 4, as said below
- sink_bias: float32 [32], P('head'), may hold values from 3 to 7
- out_weight: bfloat16 [4096, 4096], P('head'), may hold values from -0.09375 to 0.09375
Outputs:
- attn_out: bfloat16 [12288, 4096], P(('seq', 'head'))
The draws below stay inside these ranges and needn't reach their ends.
Inputs may be any that keep to these rules, and one draw needn't show every extreme that they name: `windows`: each head's window lies between 768 and 1536, and some head has exactly 1536. `sink_counts`: each head has 1 to 4 sink tokens, and some head has exactly 4.
All inputs are finite; a program needn't handle non-finite values.
Results may differ from the reference program's by a relative error of at most 0.018.
Values may be sent and summed in bfloat16 or wider, within the bound.
No kernel may reach another device: no remote copies, remote signals or barrier semaphores. Data moves between devices by JAX's collectives and lax.ppermute only.
A program may use at most 64 MiB of HBM per device.

```python
import jax
import jax.numpy as jnp
from jax import lax

D = 4096
H = 32
KVH = 8
HD = 128
WINDOW = 1536
SINKS = 4
TOK_DEV = 192
TOKENS = 12288
N_SEQ = 64
N_HEAD = 8


def shared_keys(key):
    return jnp.clip(jax.random.normal(jax.random.fold_in(key, 11), (TOKENS, KVH, HD), jnp.float32), -4.5, 4.5)


def draw_key_rows(key, part):
    return shared_keys(key).astype(jnp.bfloat16)


def draw_queries(key, part):
    base = jnp.clip(jax.random.normal(jax.random.fold_in(key, 12), (TOKENS, H, HD), jnp.float32), -4.5, 4.5)
    return base.astype(jnp.bfloat16)


def draw_windows(key, part):
    spread = jax.random.randint(jax.random.fold_in(key, 21), (H,), WINDOW // 2, WINDOW + 1)
    chosen = jax.random.randint(jax.random.fold_in(key, 22), (), 0, H)
    return jnp.where(jnp.arange(H) == chosen, WINDOW, spread).astype(jnp.int32)


def draw_sink_counts(key, part):
    spread = jax.random.randint(jax.random.fold_in(key, 31), (H,), 1, SINKS + 1)
    chosen = jax.random.randint(jax.random.fold_in(key, 32), (), 0, H)
    return jnp.where(jnp.arange(H) == chosen, SINKS, spread).astype(jnp.int32)


def steps_of(stream_key, dims, split, least, high):
    def one(dim, blocks):
        draws = jax.random.uniform(jax.random.fold_in(jax.random.fold_in(stream_key, 6), dim), (blocks,), jnp.float32, least / len(split), high / len(split))
        return jnp.repeat(jnp.exp(draws), dims[dim] // blocks).reshape((-1,) + (1,) * (len(dims) - dim - 1))

    level = one(*split[0])
    for cut in split[1:]:
        level = level * one(*cut)
    return level


def noise(own_key, extent, scale, most, pieces=(), held_as=jnp.bfloat16):
    values = jax.random.normal(own_key, extent, jnp.float32) * scale
    if len(pieces) > 0:
        values = steps_of(own_key, extent, pieces, -0.22, 0.18) * values
    return jnp.clip(values, min=-most, max=most).astype(held_as)


def setup_inputs(seed: int = 0) -> dict:
    streams_of = jax.random.split(jax.random.key(seed), 8)
    return {
        "queries": draw_queries(jax.random.fold_in(streams_of[7], 71), 0),
        "key_rows": draw_key_rows(jax.random.fold_in(streams_of[7], 71), 0),
        "value_rows": noise(streams_of[2], (TOKENS, KVH, HD), 4.0, 24.0, ((0, 64), (1, 8))),
        "windows": draw_windows(jax.random.fold_in(streams_of[7], 71), 0),
        "sink_counts": draw_sink_counts(jax.random.fold_in(streams_of[7], 71), 0),
        "sink_bias": jnp.clip(3.0 + 4.0 * jax.random.uniform(streams_of[5], (H,), jnp.float32) ** steps_of(streams_of[5], (H,), ((0, 8),), -0.2, 0.2), 3.0, 7.0),
        "out_weight": noise(streams_of[6], (H * HD, D), (H * HD) ** -0.5, 0.09375, ((0, 8),)),
    }


def attend_block(query_block, band_rows, sink_rows, first_pos, windows, sink_counts, sink_bias):
    tok_rows, local_heads, head_width = query_block.shape
    kv_local = band_rows.shape[2]
    group_size = local_heads // kv_local
    band_span = band_rows.shape[1]
    all_keys = jnp.concatenate([sink_rows[0], band_rows[0]], axis=0)
    all_values = jnp.concatenate([sink_rows[1], band_rows[1]], axis=0)
    grouped = query_block.reshape(tok_rows, kv_local, group_size, head_width)
    score_scale = 1.0 / (head_width ** 0.5)
    scores = jnp.einsum("tkgd,skd->kgts", grouped.astype(jnp.float32), all_keys.astype(jnp.float32)) * score_scale
    query_pos = first_pos + jnp.arange(tok_rows, dtype=jnp.int32)
    band_pos = first_pos + tok_rows - band_span + jnp.arange(band_span, dtype=jnp.int32)
    sink_pos = jnp.arange(SINKS, dtype=jnp.int32)
    key_pos = jnp.concatenate([sink_pos, band_pos])
    is_sink = jnp.concatenate([jnp.ones((SINKS,), bool), jnp.zeros((band_span,), bool)])
    head_window = windows.reshape(kv_local, group_size, 1, 1)
    head_sinks = sink_counts.reshape(kv_local, group_size, 1, 1)
    head_bias = sink_bias.reshape(kv_local, group_size, 1, 1)
    distance = query_pos[:, None] - key_pos[None, :]
    visible = (distance >= 0) & jnp.where(is_sink, key_pos < head_sinks, (distance < head_window) & (key_pos >= head_sinks))
    scores = scores + jnp.where(is_sink, head_bias, 0.0)
    masked = jnp.where(visible, scores, -1e30)
    highest = jnp.max(masked, axis=-1, keepdims=True)
    weights = jnp.where(visible, jnp.exp(masked - highest), 0.0)
    normed = (weights / jnp.sum(weights, axis=-1, keepdims=True)).astype(jnp.bfloat16)
    mixed = jnp.einsum("kgts,skd->tkgd", normed.astype(jnp.float32), all_values.astype(jnp.float32))
    return mixed.astype(jnp.bfloat16).reshape(tok_rows, local_heads * head_width)


def reference(queries, key_rows, value_rows, windows, sink_counts, sink_bias, out_weight):
    stacked = jnp.stack([key_rows, value_rows])
    padding = jnp.zeros((2, WINDOW, KVH, HD), jnp.bfloat16)
    padded = jnp.concatenate([padding, stacked], axis=1)
    sink_rows = stacked[:, :SINKS]

    def one_shard(shard_index):
        first_pos = (shard_index * TOK_DEV).astype(jnp.int32)
        query_block = lax.dynamic_slice_in_dim(queries, first_pos, TOK_DEV, 0)
        band_rows = lax.dynamic_slice_in_dim(padded, first_pos, TOK_DEV + WINDOW, 1)
        return attend_block(query_block, band_rows, sink_rows, first_pos, windows, sink_counts, sink_bias)

    attended = lax.map(one_shard, jnp.arange(N_SEQ, dtype=jnp.int32)).reshape(TOKENS, H * HD)
    group_rows = H * HD // N_HEAD
    total = jnp.zeros((TOKENS, D), jnp.float32)
    for member in range(N_HEAD):
        lower = member * group_rows
        term = jnp.dot(attended[:, lower:lower + group_rows], out_weight[lower:lower + group_rows], preferred_element_type=jnp.float32)
        total = total + lax.optimization_barrier(term.astype(jnp.bfloat16)).astype(jnp.float32)
    return total.astype(jnp.bfloat16)
```

```python
import functools

import jax
import jax.numpy as jnp
from jax import lax
from jax.experimental import pallas as pl
from jax.experimental.pallas import tpu as pltpu
from jax.sharding import Mesh
from jax.sharding import PartitionSpec as P

WINDOW = 1536
SINKS = 4
SEQ = ("zh", "x", "y")
HEAD = ("zl", "core")
LANES = 128
NEG = -1e30
LOG2E = 1.4426950408889634
ALWAYS, NEVER = 1 << 30, -(1 << 30)


def attend_kernel(place, win, cnt, bias, q_ref, halo_ref, near_ref, out_ref, *, tok_rows, row_len):
    heads, rows, width = q_ref.shape[1:]
    first_pos, y, part = place[0], place[1], place[2]
    unit = LOG2E / width**0.5
    halo_len = row_len * tok_rows
    near_len = near_ref.shape[1]
    row = lax.broadcasted_iota(jnp.int32, (rows, 1), 0)
    per = rows // 4
    jump = sum((row >= per * k).astype(jnp.int32) for k in range(1, 4))
    tok = row + jump * per + part * per
    query_pos = first_pos + tok
    row_start = first_pos - y * tok_rows
    number = lax.broadcasted_iota(jnp.int32, (1, halo_len), 1)
    halo_pos = row_start + number - jnp.where(number < y * tok_rows, 0, halo_len)
    near = lax.broadcasted_iota(jnp.int32, (1, near_len), 1)
    is_sink = near >= tok_rows
    near_pos = jnp.where(is_sink, near - tok_rows, first_pos + near)
    keys = halo_ref[:, 0].reshape(halo_len, width)
    values = halo_ref[:, 1].reshape(halo_len, width)
    near_keys, near_values = near_ref[0], near_ref[1]
    transposed = (((1,), (1,)), ((), ()))
    for h in range(heads):
        q = q_ref[part, h]
        lowest = jnp.maximum(query_pos - win[h] + 1, cnt[h])
        far = lax.dot_general(q, keys, transposed, preferred_element_type=jnp.float32)
        far = jnp.where(halo_pos >= lowest, far, NEG)
        close = lax.dot_general(q, near_keys, transposed, preferred_element_type=jnp.float32)
        close = close + jnp.where(is_sink, bias[h] * (width**0.5), 0.0)
        ranked = jnp.where(is_sink, jnp.where(near_pos < cnt[h], ALWAYS, NEVER), near_pos)
        close = jnp.where((near_pos <= query_pos) & (ranked >= lowest), close, NEG)
        top = jnp.maximum(
            jnp.max(far, axis=1, keepdims=True), jnp.max(close, axis=1, keepdims=True)
        )
        far = jnp.exp2((far - top) * unit)
        close = jnp.exp2((close - top) * unit)
        total = jnp.sum(far, axis=1, keepdims=True) + jnp.sum(close, axis=1, keepdims=True)
        mixed = jnp.dot(far.astype(jnp.bfloat16), values, preferred_element_type=jnp.float32)
        mixed += jnp.dot(
            close.astype(jnp.bfloat16), near_values, preferred_element_type=jnp.float32
        )
        out_ref[:, h * width : (h + 1) * width] = (mixed / total).astype(out_ref.dtype)


def attend(place, windows, sink_counts, sink_bias, q, halo, near):
    heads, rows, width = q.shape[1:]
    tok_rows = halo.shape[2]
    row_len = halo.shape[0]
    smem = pl.BlockSpec(memory_space=pltpu.SMEM)
    vmem = pl.BlockSpec(memory_space=pltpu.VMEM)
    span = row_len * tok_rows + near.shape[1]
    return pl.pallas_call(
        functools.partial(attend_kernel, tok_rows=tok_rows, row_len=row_len),
        out_shape=jax.ShapeDtypeStruct((rows, heads * width), jnp.bfloat16),
        in_specs=[smem] * 4 + [vmem] * 3,
        out_specs=vmem,
        cost_estimate=pl.CostEstimate(
            flops=4 * heads * rows * span * width,
            bytes_accessed=halo.size * 2,
            transcendentals=heads * rows * span,
        ),
        name="attend",
    )(place, windows, sink_counts, sink_bias, q, halo, near)


def shards(queries, key_rows, value_rows, windows, sink_counts, sink_bias, out_weight):
    tok_rows, heads, width = queries.shape
    row_len = lax.axis_size("y")
    seq_len = lax.axis_size(SEQ)
    y, core = lax.axis_index("y"), lax.axis_index("core")
    first_pos = lax.axis_index(SEQ) * tok_rows
    stacked = jnp.stack([key_rows[:, 0], value_rows[:, 0]])
    before = lax.ppermute(stacked, SEQ, [(i, i + row_len) for i in range(seq_len - row_len)])
    other_weight = lax.ppermute(out_weight, "core", [(0, 1), (1, 0)])
    sinks = stacked[:, :SINKS]
    sinks = lax.all_to_all(
        jnp.broadcast_to(sinks[None], (row_len, *sinks.shape)), "y", 0, 0, tiled=True
    )[0]
    rows_of = lax.axis_size(("zh", "x"))
    sinks = lax.all_to_all(
        jnp.broadcast_to(sinks[None], (rows_of, *sinks.shape)), ("zh", "x"), 0, 0, tiled=True
    )[0]
    target = lax.broadcasted_iota(jnp.int32, (row_len, 1, 1, 1), 0)
    sent = jnp.where(target > y, stacked[None], before[None])
    halo = lax.all_to_all(sent, "y", 0, 0, tiled=True)
    near = jnp.concatenate(
        [stacked, jnp.pad(sinks, ((0, 0), (0, 64 - SINKS), (0, 0)))], axis=1
    )
    members, cores = lax.axis_size("zl"), lax.axis_size("core")
    own = tok_rows // (members * cores)
    q = queries.reshape(members, cores, own, heads, width)
    q = q.transpose(1, 3, 0, 2, 4).reshape(cores, heads, members * own, width)

    def attended(part):
        place = jnp.stack([first_pos, y, part]).astype(jnp.int32)
        return attend(place, windows, sink_counts, sink_bias, q, halo, near)

    theirs = lax.ppermute(attended(1 - core), "core", [(0, 1), (1, 0)])
    mine = attended(core)
    summed = jnp.dot(mine, out_weight, preferred_element_type=jnp.float32) + jnp.dot(
        theirs, other_weight, preferred_element_type=jnp.float32
    )
    parts = summed.astype(jnp.bfloat16).reshape(members, own, -1)
    arrived = lax.all_to_all(parts, "zl", 0, 0, tiled=True)
    return arrived.astype(jnp.float32).sum(axis=0).astype(jnp.bfloat16)


def solution(mesh):
    split = Mesh(mesh.devices.reshape(2, 4, 8, 4, 2), SEQ + HEAD)
    return jax.shard_map(
        shards,
        mesh=split,
        in_specs=(
            P(SEQ, HEAD, None),
            P(SEQ, HEAD, None),
            P(SEQ, HEAD, None),
            P(HEAD),
            P(HEAD),
            P(HEAD),
            P(HEAD, None),
        ),
        out_specs=P(SEQ + HEAD, None),
        check_vma=False,
    )
```

```python
import functools

import jax
import jax.numpy as jnp
from jax import lax
from jax.experimental import pallas as pl
from jax.experimental.pallas import tpu as pltpu
from jax.sharding import Mesh
from jax.sharding import PartitionSpec as P

SINKS = 4
SEQ = ("zh", "x", "y")
HEAD = ("zl", "core")
NEG = -1e30
LOG2E = 1.4426950408889634
SPREAD = (("zh", [(0, 1)]), ("x", [(0, 1)]), ("x", [(0, 2), (1, 3)]))
ALWAYS, NEVER = 1 << 30, -(1 << 30)


def attend_kernel(place, win, cnt, bias, q_ref, halo_ref, near_ref, out_ref, *, tok_rows, row_len):
    heads, rows, width = q_ref.shape[1:]
    first_pos, y, part = place[0], place[1], place[2]
    unit = LOG2E / width**0.5
    halo_len = row_len * tok_rows
    near_len = near_ref.shape[1]
    row = lax.broadcasted_iota(jnp.int32, (rows, 1), 0)
    per = rows // 4
    jump = sum((row >= per * k).astype(jnp.int32) for k in range(1, 4))
    tok = row + jump * per + part * per
    query_pos = first_pos + tok
    row_start = first_pos - y * tok_rows
    number = lax.broadcasted_iota(jnp.int32, (1, halo_len), 1)
    halo_pos = row_start + number - jnp.where(number < y * tok_rows, 0, halo_len)
    near = lax.broadcasted_iota(jnp.int32, (1, near_len), 1)
    is_sink = near >= tok_rows
    near_pos = jnp.where(is_sink, near - tok_rows, first_pos + near)
    keys = halo_ref[:, 0].reshape(halo_len, width)
    values = halo_ref[:, 1].reshape(halo_len, width)
    near_keys, near_values = near_ref[0], near_ref[1]
    transposed = (((1,), (1,)), ((), ()))
    for h in range(heads):
        q = q_ref[part, h]
        lowest = jnp.maximum(query_pos - win[h] + 1, cnt[h])
        far = lax.dot_general(q, keys, transposed, preferred_element_type=jnp.float32)
        far = jnp.where(halo_pos >= lowest, far, NEG)
        close = lax.dot_general(q, near_keys, transposed, preferred_element_type=jnp.float32)
        close = close + jnp.where(is_sink, bias[h] * (width**0.5), 0.0)
        ranked = jnp.where(is_sink, jnp.where(near_pos < cnt[h], ALWAYS, NEVER), near_pos)
        close = jnp.where((near_pos <= query_pos) & (ranked >= lowest), close, NEG)
        top = jnp.maximum(
            jnp.max(far, axis=1, keepdims=True), jnp.max(close, axis=1, keepdims=True)
        )
        far = jnp.exp2((far - top) * unit)
        close = jnp.exp2((close - top) * unit)
        total = jnp.sum(far, axis=1, keepdims=True) + jnp.sum(close, axis=1, keepdims=True)
        mixed = jnp.dot(far.astype(jnp.bfloat16), values, preferred_element_type=jnp.float32)
        mixed += jnp.dot(
            close.astype(jnp.bfloat16), near_values, preferred_element_type=jnp.float32
        )
        out_ref[:, h * width : (h + 1) * width] = (mixed / total).astype(out_ref.dtype)


def attend(place, windows, sink_counts, sink_bias, q, halo, near):
    heads, rows, width = q.shape[1:]
    tok_rows = halo.shape[2]
    row_len = halo.shape[0]
    smem = pl.BlockSpec(memory_space=pltpu.SMEM)
    vmem = pl.BlockSpec(memory_space=pltpu.VMEM)
    span = row_len * tok_rows + near.shape[1]
    return pl.pallas_call(
        functools.partial(attend_kernel, tok_rows=tok_rows, row_len=row_len),
        out_shape=jax.ShapeDtypeStruct((rows, heads * width), jnp.bfloat16),
        in_specs=[smem] * 4 + [vmem] * 3,
        out_specs=vmem,
        cost_estimate=pl.CostEstimate(
            flops=4 * heads * rows * span * width,
            bytes_accessed=halo.size * 2,
            transcendentals=heads * rows * span,
        ),
        compiler_params=pltpu.CompilerParams(vmem_limit_bytes=16 << 20),
        name="attend",
    )(place, windows, sink_counts, sink_bias, q, halo, near)


def shards(queries, key_rows, value_rows, windows, sink_counts, sink_bias, out_weight):
    tok_rows, heads, width = queries.shape
    row_len = lax.axis_size("y")
    seq_len = lax.axis_size(SEQ)
    y, core = lax.axis_index("y"), lax.axis_index("core")
    first_pos = lax.axis_index(SEQ) * tok_rows
    stacked = jnp.stack([key_rows[:, 0], value_rows[:, 0]])
    before = lax.ppermute(stacked, SEQ, [(i, i + row_len) for i in range(seq_len - row_len)])
    other_weight = lax.ppermute(out_weight, "core", [(0, 1), (1, 0)])
    sinks = stacked[:, :SINKS]
    sinks = jnp.broadcast_to(sinks[None], (row_len, *sinks.shape))
    sinks = lax.all_to_all(sinks, "y", 0, 0, tiled=True)[0]
    sinks = jnp.where(lax.axis_index(("zh", "x")) == 0, sinks, jnp.zeros_like(sinks))
    for axis, route in SPREAD:
        sinks = sinks + lax.ppermute(sinks, axis, route)
    target = lax.broadcasted_iota(jnp.int32, (row_len, 1, 1, 1), 0)
    sent = jnp.where(target > y, stacked[None], before[None])
    halo = lax.all_to_all(sent, "y", 0, 0, tiled=True)
    near = jnp.concatenate(
        [stacked, jnp.pad(sinks, ((0, 0), (0, 64 - SINKS), (0, 0)))], axis=1
    )
    members, cores = lax.axis_size("zl"), lax.axis_size("core")
    own = tok_rows // (members * cores)
    q = queries.reshape(members, cores, own, heads, width)
    q = q.transpose(1, 3, 0, 2, 4).reshape(cores, heads, members * own, width)

    def attended(part):
        place = jnp.stack([first_pos, y, part]).astype(jnp.int32)
        return attend(place, windows, sink_counts, sink_bias, q, halo, near)

    theirs = lax.ppermute(attended(1 - core), "core", [(0, 1), (1, 0)])
    mine = attended(core)
    summed = jnp.dot(mine, out_weight, preferred_element_type=jnp.float32) + jnp.dot(
        theirs, other_weight, preferred_element_type=jnp.float32
    )
    parts = summed.astype(jnp.bfloat16).reshape(members, own, -1)
    arrived = lax.all_to_all(parts, "zl", 0, 0, tiled=True)
    return arrived.astype(jnp.float32).sum(axis=0).astype(jnp.bfloat16)


def solution(mesh):
    split = Mesh(mesh.devices.reshape(2, 4, 8, 4, 2), SEQ + HEAD)
    return jax.shard_map(
        shards,
        mesh=split,
        in_specs=(
            P(SEQ, HEAD, None),
            P(SEQ, HEAD, None),
            P(SEQ, HEAD, None),
            P(HEAD),
            P(HEAD),
            P(HEAD),
            P(HEAD, None),
        ),
        out_specs=P(SEQ + HEAD, None),
        check_vma=False,
    )
```

```python
import functools

import jax
import jax.numpy as jnp
from jax import lax
from jax.experimental import pallas as pl
from jax.experimental.pallas import tpu as pltpu
from jax.sharding import Mesh
from jax.sharding import PartitionSpec as P

SINKS = 4
SEQ = ("zh", "x", "y")
HEAD = ("zl", "core")
NEG = -1e30
LOG2E = 1.4426950408889634
SPREAD = tuple(
    (SEQ, [(i, i + step) for i in range(0, 8, 2 * step)]) for step in (4, 2, 1)
) + (
    (SEQ, [(i, i + 32) for i in range(8)]),
    ("x", [(0, 1)]),
    ("x", [(0, 2), (1, 3)]),
)
ALWAYS, NEVER = 1 << 30, -(1 << 30)


def attend_kernel(table, bias, q_ref, halo_ref, near_ref, *refs, tok_rows, row_len, number):
    fetch = None
    if number == 1:
        weight_ref, out_ref, held_ref, done = refs
        fetch = pltpu.make_async_copy(weight_ref, held_ref, done)
        fetch.start()
    else:
        (out_ref,) = refs
    heads, rows, width = q_ref.shape[1:]
    first_pos, y, part = table[0], table[1], table[2 + number]
    unit = LOG2E / width**0.5
    halo_len = row_len * tok_rows
    near_len = near_ref.shape[1]
    row = lax.broadcasted_iota(jnp.int32, (rows, 1), 0)
    per = rows // 4
    jump = sum((row >= per * k).astype(jnp.int32) for k in range(1, 4))
    tok = row + jump * per + part * per
    query_pos = first_pos + tok
    row_start = first_pos - y * tok_rows
    number = lax.broadcasted_iota(jnp.int32, (1, halo_len), 1)
    halo_pos = row_start + number - jnp.where(number < y * tok_rows, 0, halo_len)
    near = lax.broadcasted_iota(jnp.int32, (1, near_len), 1)
    is_sink = near >= tok_rows
    near_pos = jnp.where(is_sink, near - tok_rows, first_pos + near)
    keys = halo_ref[:, 0].reshape(halo_len, width)
    values = halo_ref[:, 1].reshape(halo_len, width)
    near_keys, near_values = near_ref[0], near_ref[1]
    transposed = (((1,), (1,)), ((), ()))
    for h in range(heads):
        q = q_ref[part, h]
        count = table[4 + heads + h]
        lowest = jnp.maximum(query_pos - table[4 + h] + 1, count)
        far = lax.dot_general(q, keys, transposed, preferred_element_type=jnp.float32)
        far = jnp.where(halo_pos >= lowest, far, NEG)
        close = lax.dot_general(q, near_keys, transposed, preferred_element_type=jnp.float32)
        close = close + jnp.where(is_sink, bias[h], 0.0)
        ranked = jnp.where(is_sink, jnp.where(near_pos < count, ALWAYS, NEVER), near_pos)
        close = jnp.where((near_pos <= query_pos) & (ranked >= lowest), close, NEG)
        top = jnp.maximum(
            jnp.max(far, axis=1, keepdims=True), jnp.max(close, axis=1, keepdims=True)
        )
        far = jnp.exp2((far - top) * unit)
        close = jnp.exp2((close - top) * unit)
        total = jnp.sum(far, axis=1, keepdims=True) + jnp.sum(close, axis=1, keepdims=True)
        mixed = jnp.dot(far.astype(jnp.bfloat16), values, preferred_element_type=jnp.float32)
        mixed += jnp.dot(
            close.astype(jnp.bfloat16), near_values, preferred_element_type=jnp.float32
        )
        out_ref[:, h * width : (h + 1) * width] = (mixed / total).astype(out_ref.dtype)
    if fetch is not None:
        fetch.wait()


def attend(number, table, sink_bias, q, halo, near, *weights):
    heads, rows, width = q.shape[1:]
    tok_rows = halo.shape[2]
    row_len = halo.shape[0]
    smem = pl.BlockSpec(memory_space=pltpu.SMEM)
    vmem = pl.BlockSpec(memory_space=pltpu.VMEM)
    span = row_len * tok_rows + near.shape[1]
    return pl.pallas_call(
        functools.partial(attend_kernel, tok_rows=tok_rows, row_len=row_len, number=number),
        out_shape=[jax.ShapeDtypeStruct((rows, heads * width), jnp.bfloat16)]
        + [jax.ShapeDtypeStruct(w.shape, w.dtype) for w in weights],
        in_specs=[smem] * 2
        + [vmem] * 3
        + [pl.BlockSpec(memory_space=pl.ANY) for _ in weights],
        out_specs=[vmem] * (1 + len(weights)),
        scratch_shapes=[pltpu.SemaphoreType.DMA for _ in weights],
        cost_estimate=pl.CostEstimate(
            flops=4 * heads * rows * span * width,
            bytes_accessed=halo.size * 2,
            transcendentals=heads * rows * span,
        ),
        compiler_params=pltpu.CompilerParams(vmem_limit_bytes=16 << 20),
        name="attend",
    )(table, sink_bias, q, halo, near, *weights)


def shards(queries, key_rows, value_rows, windows, sink_counts, sink_bias, out_weight):
    tok_rows, heads, width = queries.shape
    row_len = lax.axis_size("y")
    seq_len = lax.axis_size(SEQ)
    y, core = lax.axis_index("y"), lax.axis_index("core")
    first_pos = lax.axis_index(SEQ) * tok_rows
    stacked = jnp.stack([key_rows[:, 0], value_rows[:, 0]])
    before = lax.ppermute(stacked, SEQ, [(i, i + row_len) for i in range(seq_len - row_len)])
    other_weight = lax.ppermute(out_weight, "core", [(0, 1), (1, 0)])
    sinks = jnp.where(lax.axis_index(SEQ) == 0, stacked[:, :SINKS], 0)
    for axis, route in SPREAD:
        sinks = sinks + lax.ppermute(sinks, axis, route)
    target = lax.broadcasted_iota(jnp.int32, (row_len, 1, 1, 1), 0)
    sent = jnp.where(target > y, stacked[None], before[None])
    halo = lax.all_to_all(sent, "y", 0, 0, tiled=True)
    near = jnp.concatenate(
        [stacked, jnp.pad(sinks, ((0, 0), (0, 64 - SINKS), (0, 0)))], axis=1
    )
    members, cores = lax.axis_size("zl"), lax.axis_size("core")
    own = tok_rows // (members * cores)
    q = queries.reshape(members, cores, own, heads, width)
    q = q.transpose(1, 3, 0, 2, 4).reshape(cores, heads, members * own, width)

    place = jnp.stack([first_pos, y, 1 - core, core]).astype(jnp.int32)
    table = jnp.concatenate([place, windows, sink_counts])
    halo, other_weight = lax.optimization_barrier((halo, other_weight))
    bias = sink_bias * width**0.5
    (theirs,) = attend(0, table, bias, q, halo, near)
    theirs = lax.ppermute(theirs, "core", [(0, 1), (1, 0)])
    mine, other_weight = attend(1, table, bias, q, halo, near, other_weight)
    summed = jnp.dot(mine, out_weight, preferred_element_type=jnp.float32) + jnp.dot(
        theirs, other_weight, preferred_element_type=jnp.float32
    )
    parts = summed.astype(jnp.bfloat16).reshape(members, own, -1)
    arrived = lax.all_to_all(parts, "zl", 0, 0, tiled=True)
    return arrived.astype(jnp.float32).sum(axis=0).astype(jnp.bfloat16)


def solution(mesh):
    split = Mesh(mesh.devices.reshape(2, 4, 8, 4, 2), SEQ + HEAD)
    return jax.shard_map(
        shards,
        mesh=split,
        in_specs=(
            P(SEQ, HEAD, None),
            P(SEQ, HEAD, None),
            P(SEQ, HEAD, None),
            P(HEAD),
            P(HEAD),
            P(HEAD),
            P(HEAD, None),
        ),
        out_specs=P(SEQ + HEAD, None),
        check_vma=False,
    )
```

```python
import functools

import jax
import jax.numpy as jnp
from jax import lax
from jax.experimental import pallas as pl
from jax.experimental.pallas import tpu as pltpu
from jax.sharding import Mesh
from jax.sharding import PartitionSpec as P

SINKS = 4
SEQ = ("zh", "x", "y")
HEAD = ("zl", "core")
NEG = -1e30
LOG2E = 1.4426950408889634
SPREAD = (
    (SEQ, [(0, 32)]),
    (SEQ, [(i, i + 8) for i in (0, 32)]),
    (SEQ, [(i, i + j) for i in (0, 32) for i, j in ((i, 24), (i + 8, 8))]),
    ("y", [(0, 1)]),
    ("y", [(0, 7), (1, 2)]),
    ("y", [(7, 5), (0, 6), (1, 3), (2, 4)]),
)
ALWAYS, NEVER = 1 << 30, -(1 << 30)


def attend_kernel(table, bias, q_ref, halo_ref, near_ref, out_ref, *, tok_rows, row_len, number):
    heads, rows, width = q_ref.shape[1:]
    first_pos, y, part = table[0], table[1], table[2 + number]
    unit = LOG2E / width**0.5
    halo_len = row_len * tok_rows
    near_len = near_ref.shape[1]
    row = lax.broadcasted_iota(jnp.int32, (rows, 1), 0)
    per = rows // 4
    jump = sum((row >= per * k).astype(jnp.int32) for k in range(1, 4))
    tok = row + jump * per + part * per
    query_pos = first_pos + tok
    row_start = first_pos - y * tok_rows
    number = lax.broadcasted_iota(jnp.int32, (1, halo_len), 1)
    halo_pos = row_start + number - jnp.where(number < y * tok_rows, 0, halo_len)
    near = lax.broadcasted_iota(jnp.int32, (1, near_len), 1)
    is_sink = near >= tok_rows
    near_pos = jnp.where(is_sink, near - tok_rows, first_pos + near)
    keys = halo_ref[:, 0].reshape(halo_len, width)
    values = halo_ref[:, 1].reshape(halo_len, width)
    near_keys, near_values = near_ref[0], near_ref[1]
    transposed = (((1,), (1,)), ((), ()))
    for h in range(heads):
        q = q_ref[part, h]
        count = table[4 + heads + h]
        lowest = jnp.maximum(query_pos - table[4 + h] + 1, count)
        far = lax.dot_general(q, keys, transposed, preferred_element_type=jnp.float32)
        far = jnp.where(halo_pos >= lowest, far, NEG)
        close = lax.dot_general(q, near_keys, transposed, preferred_element_type=jnp.float32)
        close = close + jnp.where(is_sink, bias[h], 0.0)
        ranked = jnp.where(is_sink, jnp.where(near_pos < count, ALWAYS, NEVER), near_pos)
        close = jnp.where((near_pos <= query_pos) & (ranked >= lowest), close, NEG)
        top = jnp.maximum(
            jnp.max(far, axis=1, keepdims=True), jnp.max(close, axis=1, keepdims=True)
        )
        far = jnp.exp2((far - top) * unit)
        close = jnp.exp2((close - top) * unit)
        total = jnp.sum(far, axis=1, keepdims=True) + jnp.sum(close, axis=1, keepdims=True)
        mixed = jnp.dot(far.astype(jnp.bfloat16), values, preferred_element_type=jnp.float32)
        mixed += jnp.dot(
            close.astype(jnp.bfloat16), near_values, preferred_element_type=jnp.float32
        )
        out_ref[:, h * width : (h + 1) * width] = (mixed / total).astype(out_ref.dtype)


def attend(number, table, sink_bias, q, halo, near):
    heads, rows, width = q.shape[1:]
    tok_rows = halo.shape[2]
    row_len = halo.shape[0]
    smem = pl.BlockSpec(memory_space=pltpu.SMEM)
    vmem = pl.BlockSpec(memory_space=pltpu.VMEM)
    span = row_len * tok_rows + near.shape[1]
    return pl.pallas_call(
        functools.partial(attend_kernel, tok_rows=tok_rows, row_len=row_len, number=number),
        out_shape=jax.ShapeDtypeStruct((rows, heads * width), jnp.bfloat16),
        in_specs=[smem] * 2 + [vmem] * 3,
        out_specs=vmem,
        cost_estimate=pl.CostEstimate(
            flops=32 * heads * rows * span * width,
            bytes_accessed=halo.size * 2,
            transcendentals=heads * rows * span,
        ),
        compiler_params=pltpu.CompilerParams(vmem_limit_bytes=16 << 20),
        name="attend",
    )(table, sink_bias, q, halo, near)


def shards(queries, key_rows, value_rows, windows, sink_counts, sink_bias, out_weight):
    tok_rows, heads, width = queries.shape
    row_len = lax.axis_size("y")
    seq_len = lax.axis_size(SEQ)
    y, core = lax.axis_index("y"), lax.axis_index("core")
    first_pos = lax.axis_index(SEQ) * tok_rows
    stacked = jnp.stack([key_rows[:, 0], value_rows[:, 0]])
    before = lax.ppermute(stacked, SEQ, [(i, i + row_len) for i in range(seq_len - row_len)])
    sinks = jnp.where(lax.axis_index(SEQ) == 0, stacked[:, :SINKS], 0)
    for axis, route in SPREAD:
        sinks = sinks + lax.ppermute(sinks, axis, route)
    target = lax.broadcasted_iota(jnp.int32, (row_len, 1, 1, 1), 0)
    sent = jnp.where(target > y, stacked[None], before[None])
    halo = lax.all_to_all(sent, "y", 0, 0, tiled=True)
    near = jnp.concatenate(
        [stacked, jnp.pad(sinks, ((0, 0), (0, 64 - SINKS), (0, 0)))], axis=1
    )
    members, cores = lax.axis_size("zl"), lax.axis_size("core")
    own = tok_rows // (members * cores)
    q = queries.reshape(members, cores, own, heads, width)
    q = q.transpose(1, 3, 0, 2, 4).reshape(cores, heads, members * own, width)

    place = jnp.stack([first_pos, y, 1 - core, core]).astype(jnp.int32)
    table = jnp.concatenate([place, windows, sink_counts])
    bias = sink_bias * width**0.5

    def projected(rows, weight):
        return jnp.dot(rows, weight, preferred_element_type=jnp.float32).astype(jnp.bfloat16)

    theirs = attend(0, table, bias, q, halo, near)
    theirs = projected(theirs, out_weight)
    theirs = lax.ppermute(theirs, "core", [(0, 1), (1, 0)])
    mine = attend(1, table, bias, q, halo, near)
    mine = projected(mine, out_weight)
    parts = (mine.astype(jnp.float32) + theirs.astype(jnp.float32)).astype(jnp.bfloat16)
    parts = parts.reshape(members, own, -1)
    arrived = lax.all_to_all(parts, "zl", 0, 0, tiled=True)
    return arrived.astype(jnp.float32).sum(axis=0).astype(jnp.bfloat16)


def solution(mesh):
    split = Mesh(mesh.devices.reshape(2, 4, 8, 4, 2), SEQ + HEAD)
    return jax.shard_map(
        shards,
        mesh=split,
        in_specs=(
            P(SEQ, HEAD, None),
            P(SEQ, HEAD, None),
            P(SEQ, HEAD, None),
            P(HEAD),
            P(HEAD),
            P(HEAD),
            P(HEAD, None),
        ),
        out_specs=P(SEQ + HEAD, None),
        check_vma=False,
    )
```

```python
import functools

import jax
import jax.numpy as jnp
from jax import lax
from jax.experimental import pallas as pl
from jax.experimental.pallas import tpu as pltpu
from jax.sharding import Mesh
from jax.sharding import PartitionSpec as P

SINKS = 4
SEQ = ("zh", "x", "y")
HEAD = ("zl", "core")
NEG = -1e30
LOG2E = 1.4426950408889634
SPREAD = (
    (SEQ, [(0, 32)]),
    (SEQ, [(i, i + 8) for i in (0, 32)]),
    (SEQ, [(i, i + j) for i in (0, 32) for i, j in ((i, 24), (i + 8, 8))]),
    ("y", [(0, 1)]),
    ("y", [(0, 7), (1, 2)]),
    ("y", [(7, 5), (0, 6), (1, 3), (2, 4)]),
)
ALWAYS, NEVER = 1 << 30, -(1 << 30)


def attend_kernel(
    table, bias, q_ref, halo_ref, near_ref, out_ref, score_ref, prob_ref, *, tok_rows, number
):
    heads, rows, width = q_ref.shape[1:]
    first_pos, y, member, part = table[0], table[1], table[2], table[3 + number]
    unit = LOG2E / width**0.5
    halo_len = halo_ref.shape[0] * tok_rows
    span = score_ref.shape[1]
    per = rows // 4
    row = lax.broadcasted_iota(jnp.int32, (rows, 1), 0)
    turn = sum((row >= per * k).astype(jnp.int32) for k in range(1, 4))
    query_pos = first_pos + (turn ^ member) * (2 * per) + part * per + row - turn * per
    row_start = first_pos - y * tok_rows
    place = lax.broadcasted_iota(jnp.int32, (1, halo_len), 1)
    halo_pos = row_start + place - jnp.where(place < y * tok_rows, 0, halo_len)
    near = lax.broadcasted_iota(jnp.int32, (1, span - halo_len), 1)
    is_sink = near >= tok_rows
    near_pos = jnp.where(is_sink, near - tok_rows, first_pos + near)
    q = q_ref[part].reshape(heads * rows, width)
    transposed = (((1,), (1,)), ((), ()))
    keys = jnp.concatenate([halo_ref[:, 0].reshape(halo_len, width), near_ref[0]], axis=0)
    score_ref[...] = lax.dot_general(q, keys, transposed, preferred_element_type=jnp.float32)
    totals = []
    for h in range(heads):
        count = table[5 + heads + h]
        lowest = jnp.maximum(query_pos - table[5 + h] + 1, count)
        ranked = jnp.where(is_sink, jnp.where(near_pos < count, ALWAYS, NEVER), near_pos)
        mine = slice(h * rows, (h + 1) * rows)
        far = jnp.where(halo_pos >= lowest, score_ref[mine, :halo_len], NEG)
        close = score_ref[mine, halo_len:] + jnp.where(is_sink, bias[h], 0.0)
        close = jnp.where((near_pos <= query_pos) & (ranked >= lowest), close, NEG)
        top = jnp.maximum(
            jnp.max(far, axis=1, keepdims=True), jnp.max(close, axis=1, keepdims=True)
        )
        far = jnp.exp2((far - top) * unit)
        close = jnp.exp2((close - top) * unit)
        totals.append(jnp.sum(far, axis=1, keepdims=True) + jnp.sum(close, axis=1, keepdims=True))
        prob_ref[mine, :halo_len] = far.astype(jnp.bfloat16)
        prob_ref[mine, halo_len:] = close.astype(jnp.bfloat16)
    values = jnp.concatenate([halo_ref[:, 1].reshape(halo_len, width), near_ref[1]], axis=0)
    mixed = jnp.dot(prob_ref[...], values, preferred_element_type=jnp.float32)
    for h in range(heads):
        block = mixed[h * rows : (h + 1) * rows] / totals[h]
        out_ref[:, h * width : (h + 1) * width] = block.astype(out_ref.dtype)


def attend(number, table, sink_bias, q, halo, near):
    heads, rows, width = q.shape[1:]
    tok_rows = halo.shape[2]
    smem = pl.BlockSpec(memory_space=pltpu.SMEM)
    vmem = pl.BlockSpec(memory_space=pltpu.VMEM)
    span = halo.shape[0] * tok_rows + near.shape[1]
    return pl.pallas_call(
        functools.partial(attend_kernel, tok_rows=tok_rows, number=number),
        out_shape=jax.ShapeDtypeStruct((rows, heads * width), jnp.bfloat16),
        in_specs=[smem] * 2 + [vmem] * 3,
        out_specs=vmem,
        scratch_shapes=[
            pltpu.VMEM((heads * rows, span), jnp.float32),
            pltpu.VMEM((heads * rows, span), jnp.bfloat16),
        ],
        cost_estimate=pl.CostEstimate(
            flops=32 * heads * rows * span * width,
            bytes_accessed=halo.size * 2,
            transcendentals=heads * rows * span,
        ),
        compiler_params=pltpu.CompilerParams(vmem_limit_bytes=20 << 20),
        name="attend",
    )(table, sink_bias, q, halo, near)


def project_kernel(rows_ref, weight_ref, theirs_ref, *out_refs):
    per = out_refs[0].shape[0]
    step = 512

    @pl.loop(0, weight_ref.shape[1] // step)
    def _(k):
        columns = pl.ds(pl.multiple_of(k * step, step), step)
        total = jnp.dot(rows_ref[...], weight_ref[:, columns], preferred_element_type=jnp.float32)
        total = total.astype(jnp.bfloat16).astype(jnp.float32)
        total = total + theirs_ref[:, columns].astype(jnp.float32)
        for number, out_ref in enumerate(out_refs):
            out_ref[:, columns] = total[number * per : (number + 1) * per].astype(out_ref.dtype)


def project(rows, weight, theirs, members):
    vmem = pl.BlockSpec(memory_space=pltpu.VMEM)
    per, columns = rows.shape[0] // members, weight.shape[1]
    return pl.pallas_call(
        project_kernel,
        out_shape=[jax.ShapeDtypeStruct((per, columns), jnp.bfloat16)] * members,
        in_specs=[vmem] * 3,
        out_specs=[vmem] * members,
        cost_estimate=pl.CostEstimate(
            flops=2 * rows.size * columns, bytes_accessed=weight.size * 2, transcendentals=0
        ),
        compiler_params=pltpu.CompilerParams(vmem_limit_bytes=20 << 20),
        name="project",
    )(rows, weight, theirs)


def shards(queries, key_rows, value_rows, windows, sink_counts, sink_bias, out_weight):
    tok_rows, heads, width = queries.shape
    row_len = lax.axis_size("y")
    seq_len = lax.axis_size(SEQ)
    y, core = lax.axis_index("y"), lax.axis_index("core")
    first_pos = lax.axis_index(SEQ) * tok_rows
    stacked = jnp.stack([key_rows[:, 0], value_rows[:, 0]])
    before = lax.ppermute(stacked, SEQ, [(i, i + row_len) for i in range(seq_len - row_len)])
    sinks = jnp.where(lax.axis_index(SEQ) == 0, stacked[:, :SINKS], 0)
    for axis, route in SPREAD:
        sinks = sinks + lax.ppermute(sinks, axis, route)
    target = lax.broadcasted_iota(jnp.int32, (row_len, 1, 1, 1), 0)
    sent = jnp.where(target > y, stacked[None], before[None])
    halo = lax.all_to_all(sent, "y", 0, 0, tiled=True)
    near = jnp.concatenate(
        [stacked, jnp.pad(sinks, ((0, 0), (0, 64 - SINKS), (0, 0)))], axis=1
    )
    members, cores = lax.axis_size("zl"), lax.axis_size("core")
    own = tok_rows // (members * cores)
    member = lax.axis_index("zl")
    q = queries.reshape(2, 2, cores, own, heads, width)
    q = jnp.where(member % 2 == 1, jnp.stack([q[:, 1], q[:, 0]], axis=1), q)
    q = jnp.where(member // 2 == 1, jnp.stack([q[1], q[0]]), q)
    q = q.reshape(members, cores, own, heads, width)
    q = q.transpose(1, 3, 0, 2, 4).reshape(cores, heads, members * own, width)
    place = jnp.stack([first_pos, y, member, 1 - core, core]).astype(jnp.int32)
    table = jnp.concatenate([place, windows, sink_counts])
    bias = sink_bias * width**0.5
    theirs = attend(0, table, bias, q, halo, near)
    theirs = jnp.dot(theirs, out_weight, preferred_element_type=jnp.float32).astype(jnp.bfloat16)
    theirs = lax.ppermute(theirs, "core", [(0, 1), (1, 0)])
    mine = attend(1, table, bias, q, halo, near)
    parts = project(mine, out_weight, theirs, members)
    total = parts[0].astype(jnp.float32)
    for distance in (3, 2, 1):
        route = [(i, i ^ distance) for i in range(members)]
        total += lax.ppermute(parts[distance], "zl", route).astype(jnp.float32)
    return total.astype(jnp.bfloat16)


def solution(mesh):
    split = Mesh(mesh.devices.reshape(2, 4, 8, 4, 2), SEQ + HEAD)
    return jax.shard_map(
        shards,
        mesh=split,
        in_specs=(
            P(SEQ, HEAD, None),
            P(SEQ, HEAD, None),
            P(SEQ, HEAD, None),
            P(HEAD),
            P(HEAD),
            P(HEAD),
            P(HEAD, None),
        ),
        out_specs=P(SEQ + HEAD, None),
        check_vma=False,
    )
```

```python
import functools

import jax
import jax.numpy as jnp
from jax import lax
from jax.experimental import pallas as pl
from jax.experimental.pallas import tpu as pltpu
from jax.sharding import Mesh
from jax.sharding import PartitionSpec as P

SINKS = 4
SEQ = ("zh", "x", "y")
HEAD = ("zl", "core")
LANES = 128
NEG = -1e30
LOG2E = 1.4426950408889634
SPREAD = (
    (SEQ, [(0, 32)]),
    (SEQ, [(i, i + 8) for i in (0, 32)]),
    (SEQ, [(i, i + j) for i in (0, 32) for i, j in ((i, 24), (i + 8, 8))]),
    ("y", [(0, 1)]),
    ("y", [(0, 7), (1, 2)]),
    ("y", [(7, 5), (0, 6), (1, 3), (2, 4)]),
)
ORDER = (4, 5, 6, 7, 3, 2, 1, 0)
ALWAYS, NEVER = 1 << 30, -(1 << 30)


def listed(number):
    return sum(jnp.where(number == k, y, 0) for k, y in enumerate(ORDER))


def pack_kernel(y_ref, own_ref, before_ref, sent_ref):
    target = listed(lax.broadcasted_iota(jnp.int32, y_ref.shape, 0))
    later = (target > y_ref[...]).astype(jnp.float32).astype(jnp.bfloat16)
    for number in range(sent_ref.shape[0]):
        chosen = later[number : number + 1]
        sent_ref[number] = own_ref[...] * chosen + before_ref[...] * (1 - chosen)


def pack(y, own, before, row_len):
    vmem = pl.BlockSpec(memory_space=pltpu.VMEM)
    return pl.pallas_call(
        pack_kernel,
        out_shape=jax.ShapeDtypeStruct((row_len, *own.shape), own.dtype),
        in_specs=[vmem] * 3,
        out_specs=vmem,
        compiler_params=pltpu.CompilerParams(vmem_limit_bytes=8 << 20),
        name="pack",
    )(jnp.full((row_len, LANES), y, jnp.int32), own, before)


def attend_kernel(
    table, bias, q_ref, halo_ref, near_ref, out_ref, score_ref, prob_ref, *, tok_rows, number
):
    heads, rows, width = q_ref.shape[1:]
    first_pos, y, member, part = (table[k : k + 1, :1] for k in (0, 1, 2, 3 + number))
    unit = LOG2E / width**0.5
    halo_len = halo_ref.shape[0] * tok_rows
    span = score_ref.shape[1]
    per = rows // 4
    row = lax.broadcasted_iota(jnp.int32, (rows, 1), 0)
    turn = sum((row >= per * k).astype(jnp.int32) for k in range(1, 4))
    query_pos = first_pos + (turn ^ member) * (2 * per) + part * per + row - turn * per
    place = lax.broadcasted_iota(jnp.int32, (1, halo_len), 1)
    block = sum((place >= k * tok_rows).astype(jnp.int32) for k in range(1, len(ORDER)))
    source = listed(block)
    halo_pos = first_pos + (source - y - block) * tok_rows + place
    halo_pos = halo_pos - jnp.where(source < y, 0, halo_len)
    near = lax.broadcasted_iota(jnp.int32, (1, span - halo_len), 1)
    is_sink = near >= tok_rows
    near_pos = jnp.where(is_sink, near - tok_rows, first_pos + near)
    first = (1 - part).astype(jnp.float32).astype(jnp.bfloat16)
    q = (q_ref[0] * first + q_ref[1] * (1 - first)).reshape(heads * rows, width)
    transposed = (((1,), (1,)), ((), ()))
    keys = jnp.concatenate([halo_ref[:, 0].reshape(halo_len, width), near_ref[0]], axis=0)
    score_ref[...] = lax.dot_general(q, keys, transposed, preferred_element_type=jnp.float32)
    totals = []
    for h in range(heads):
        window, count = (table[k : k + 1, :1] for k in (5 + h, 5 + heads + h))
        lowest = jnp.maximum(query_pos - window + 1, count)
        ranked = jnp.where(is_sink, jnp.where(near_pos < count, ALWAYS, NEVER), near_pos)
        mine = slice(h * rows, (h + 1) * rows)
        far = jnp.where(halo_pos >= lowest, score_ref[mine, :halo_len], NEG)
        close = score_ref[mine, halo_len:] + jnp.where(is_sink, bias[h : h + 1, :1], 0.0)
        close = jnp.where((near_pos <= query_pos) & (ranked >= lowest), close, NEG)
        top = jnp.maximum(
            jnp.max(far, axis=1, keepdims=True), jnp.max(close, axis=1, keepdims=True)
        )
        far = jnp.exp2((far - top) * unit)
        close = jnp.exp2((close - top) * unit)
        totals.append(jnp.sum(far, axis=1, keepdims=True) + jnp.sum(close, axis=1, keepdims=True))
        prob_ref[mine, :halo_len] = far.astype(jnp.bfloat16)
        prob_ref[mine, halo_len:] = close.astype(jnp.bfloat16)
    values = jnp.concatenate([halo_ref[:, 1].reshape(halo_len, width), near_ref[1]], axis=0)
    mixed = jnp.dot(prob_ref[...], values, preferred_element_type=jnp.float32)
    for h in range(heads):
        block = mixed[h * rows : (h + 1) * rows] / totals[h]
        out_ref[:, h * width : (h + 1) * width] = block.astype(out_ref.dtype)


def attend(number, table, sink_bias, q, halo, near):
    heads, rows, width = q.shape[1:]
    tok_rows = halo.shape[2]
    vmem = pl.BlockSpec(memory_space=pltpu.VMEM)
    span = halo.shape[0] * tok_rows + near.shape[1]
    return pl.pallas_call(
        functools.partial(attend_kernel, tok_rows=tok_rows, number=number),
        out_shape=jax.ShapeDtypeStruct((rows, heads * width), jnp.bfloat16),
        in_specs=[vmem] * 5,
        out_specs=vmem,
        scratch_shapes=[
            pltpu.VMEM((heads * rows, span), jnp.float32),
            pltpu.VMEM((heads * rows, span), jnp.bfloat16),
        ],
        cost_estimate=pl.CostEstimate(
            flops=32 * heads * rows * span * width,
            bytes_accessed=halo.size * 2,
            transcendentals=heads * rows * span,
        ),
        compiler_params=pltpu.CompilerParams(vmem_limit_bytes=20 << 20),
        name="attend",
    )(table, sink_bias, q, halo, near)


def project_kernel(rows_ref, weight_ref, theirs_ref, *out_refs):
    per = out_refs[0].shape[0]
    step = 512

    for k in range(weight_ref.shape[1] // step):
        columns = slice(k * step, (k + 1) * step)
        total = jnp.dot(rows_ref[...], weight_ref[:, columns], preferred_element_type=jnp.float32)
        total = total.astype(jnp.bfloat16).astype(jnp.float32)
        total = total + theirs_ref[:, columns].astype(jnp.float32)
        for number, out_ref in enumerate(out_refs):
            out_ref[:, columns] = total[number * per : (number + 1) * per].astype(out_ref.dtype)


def project(rows, weight, theirs, members):
    vmem = pl.BlockSpec(memory_space=pltpu.VMEM)
    per, columns = rows.shape[0] // members, weight.shape[1]
    return pl.pallas_call(
        project_kernel,
        out_shape=[jax.ShapeDtypeStruct((per, columns), jnp.bfloat16)] * members,
        in_specs=[vmem] * 3,
        out_specs=[vmem] * members,
        cost_estimate=pl.CostEstimate(
            flops=2 * rows.size * columns, bytes_accessed=weight.size * 2, transcendentals=0
        ),
        compiler_params=pltpu.CompilerParams(vmem_limit_bytes=20 << 20),
        name="project",
    )(rows, weight, theirs)


def shards(queries, key_rows, value_rows, windows, sink_counts, sink_bias, out_weight):
    tok_rows, heads, width = queries.shape
    row_len = lax.axis_size("y")
    seq_len = lax.axis_size(SEQ)
    y, core = lax.axis_index("y"), lax.axis_index("core")
    first_pos = lax.axis_index(SEQ) * tok_rows
    stacked = jnp.stack([key_rows[:, 0], value_rows[:, 0]])
    before = lax.ppermute(stacked, SEQ, [(i, i + row_len) for i in range(seq_len - row_len)])
    sinks = jnp.where(lax.axis_index(SEQ) == 0, stacked[:, :SINKS], 0)
    moved = lax.ppermute(sinks, *SPREAD[0])
    sent = pack(y, stacked, before, row_len)
    halo = lax.all_to_all(sent, "y", 0, 0, axis_index_groups=[list(ORDER)], tiled=True)
    sinks, moved, windows, sink_counts, sink_bias, _ = lax.optimization_barrier(
        (sinks, moved, windows, sink_counts, sink_bias, sent)
    )
    sinks = sinks + moved
    for number, (axis, route) in enumerate(SPREAD[1:], 1):
        if number == len(SPREAD) - 1:
            sinks, queries = lax.optimization_barrier((sinks, queries))
        sinks = sinks + lax.ppermute(sinks, axis, route)
    near = jnp.concatenate(
        [stacked, jnp.pad(sinks, ((0, 0), (0, 64 - SINKS), (0, 0)))], axis=1
    )
    members, cores = lax.axis_size("zl"), lax.axis_size("core")
    own = tok_rows // (members * cores)
    member = lax.axis_index("zl")
    q = queries.reshape(2, 2, cores, own, heads, width)
    q = jnp.where(member % 2 == 1, jnp.stack([q[:, 1], q[:, 0]], axis=1), q)
    q = jnp.where(member // 2 == 1, jnp.stack([q[1], q[0]]), q)
    q = q.reshape(members, cores, own, heads, width)
    q = q.transpose(1, 3, 0, 2, 4).reshape(cores, heads, members * own, width)
    place = jnp.stack([first_pos, y, member, 1 - core, core]).astype(jnp.int32)
    table = jnp.concatenate([place, windows, sink_counts])
    table = jnp.pad(table, (0, -len(table) % 8))[:, None]
    bias = jnp.pad(sink_bias * width**0.5, (0, 8 - heads))[:, None]
    table = jnp.broadcast_to(table, (16, LANES))
    bias = jnp.broadcast_to(bias, (8, LANES))
    theirs = attend(0, table, bias, q, halo, near)
    theirs = jnp.dot(theirs, out_weight, preferred_element_type=jnp.float32).astype(jnp.bfloat16)
    theirs = lax.ppermute(theirs, "core", [(0, 1), (1, 0)])
    mine = attend(1, table, bias, q, halo, near)
    parts = project(mine, out_weight, theirs, members)
    total = parts[0].astype(jnp.float32)
    for distance in (3, 2, 1):
        route = [(i, i ^ distance) for i in range(members)]
        total += lax.ppermute(parts[distance], "zl", route).astype(jnp.float32)
    return total.astype(jnp.bfloat16)


def solution(mesh):
    split = Mesh(mesh.devices.reshape(2, 4, 8, 4, 2), SEQ + HEAD)
    return jax.shard_map(
        shards,
        mesh=split,
        in_specs=(
            P(SEQ, HEAD, None),
            P(SEQ, HEAD, None),
            P(SEQ, HEAD, None),
            P(HEAD),
            P(HEAD),
            P(HEAD),
            P(HEAD, None),
        ),
        out_specs=P(SEQ + HEAD, None),
        check_vma=False,
    )
```

```python
import functools

import jax
import jax.numpy as jnp
from jax import lax
from jax.experimental import pallas as pl
from jax.experimental.pallas import tpu as pltpu
from jax.sharding import Mesh
from jax.sharding import PartitionSpec as P

SINKS = 4
SEQ = ("zh", "x", "y")
HEAD = ("zl", "core")
LANES = 128
NEG = -1e30
LOG2E = 1.4426950408889634
SPREAD = (
    (SEQ, [(0, 1)]),
    (SEQ, [(0, 7), (1, 2)]),
    (SEQ, [(7, 5), (0, 6), (1, 3), (2, 4)]),
    (SEQ, [(i, i + 8) for i in range(8)]),
    (SEQ, [(i + j, i + k) for i in range(8) for j, k in ((0, 24), (8, 16))]),
    ("zh", [(0, 1)]),
)
ORDER = (4, 5, 6, 7, 3, 2, 1, 0)
ALWAYS, NEVER = 1 << 30, -(1 << 30)


def listed(number):
    return sum(jnp.where(number == k, y, 0) for k, y in enumerate(ORDER))


def pack_kernel(y_ref, own_ref, before_ref, sent_ref):
    target = listed(lax.broadcasted_iota(jnp.int32, y_ref.shape, 0))
    later = (target > y_ref[...]).astype(jnp.float32).astype(jnp.bfloat16)
    for number in range(sent_ref.shape[0]):
        chosen = later[number : number + 1]
        sent_ref[number] = own_ref[...] * chosen + before_ref[...] * (1 - chosen)


def pack(y, own, before, row_len):
    vmem = pl.BlockSpec(memory_space=pltpu.VMEM)
    return pl.pallas_call(
        pack_kernel,
        out_shape=jax.ShapeDtypeStruct((row_len, *own.shape), own.dtype),
        in_specs=[vmem] * 3,
        out_specs=vmem,
        compiler_params=pltpu.CompilerParams(vmem_limit_bytes=8 << 20),
        name="pack",
    )(jnp.full((row_len, LANES), y, jnp.int32), own, before)


def attend_kernel(
    table, bias, q_ref, halo_ref, near_ref, out_ref, score_ref, prob_ref, *, tok_rows, number, half
):
    heads, rows, width = q_ref.shape[1:]
    rows = rows // 2
    chosen = slice(half * rows, (half + 1) * rows)
    first_pos, y, member, part = (table[k : k + 1, :1] for k in (0, 1, 2, 3 + number))
    unit = LOG2E / width**0.5
    halo_len = halo_ref.shape[0] * tok_rows
    span = score_ref.shape[1]
    per = rows // 2
    row = lax.broadcasted_iota(jnp.int32, (rows, 1), 0)
    turn = (row >= per).astype(jnp.int32)
    query_pos = first_pos + ((turn + 2 * half) ^ member) * (2 * per)
    query_pos = query_pos + part * per + row - turn * per
    place = lax.broadcasted_iota(jnp.int32, (1, halo_len), 1)
    block = sum((place >= k * tok_rows).astype(jnp.int32) for k in range(1, len(ORDER)))
    source = listed(block)
    halo_pos = first_pos + (source - y - block) * tok_rows + place
    halo_pos = halo_pos - jnp.where(source < y, 0, halo_len)
    near = lax.broadcasted_iota(jnp.int32, (1, span - halo_len), 1)
    is_sink = near >= tok_rows
    near_pos = jnp.where(is_sink, near - tok_rows, first_pos + near)
    first = (1 - part).astype(jnp.float32).astype(jnp.bfloat16)
    q = q_ref[0, :, chosen] * first + q_ref[1, :, chosen] * (1 - first)
    q = q.reshape(heads * rows, width)
    transposed = (((1,), (1,)), ((), ()))
    keys = jnp.concatenate([halo_ref[:, 0].reshape(halo_len, width), near_ref[0]], axis=0)
    score_ref[...] = lax.dot_general(q, keys, transposed, preferred_element_type=jnp.float32)
    totals = []
    for h in range(heads):
        window, count = (table[k : k + 1, :1] for k in (5 + h, 5 + heads + h))
        lowest = jnp.maximum(query_pos - window + 1, count)
        ranked = jnp.where(is_sink, jnp.where(near_pos < count, ALWAYS, NEVER), near_pos)
        mine = slice(h * rows, (h + 1) * rows)
        far = jnp.where(halo_pos >= lowest, score_ref[mine, :halo_len], NEG)
        close = score_ref[mine, halo_len:] + jnp.where(is_sink, bias[h : h + 1, :1], 0.0)
        close = jnp.where((near_pos <= query_pos) & (ranked >= lowest), close, NEG)
        top = jnp.maximum(
            jnp.max(far, axis=1, keepdims=True), jnp.max(close, axis=1, keepdims=True)
        )
        far = jnp.exp2((far - top) * unit)
        close = jnp.exp2((close - top) * unit)
        totals.append(jnp.sum(far, axis=1, keepdims=True) + jnp.sum(close, axis=1, keepdims=True))
        prob_ref[mine, :halo_len] = far.astype(jnp.bfloat16)
        prob_ref[mine, halo_len:] = close.astype(jnp.bfloat16)
    values = jnp.concatenate([halo_ref[:, 1].reshape(halo_len, width), near_ref[1]], axis=0)
    mixed = jnp.dot(prob_ref[...], values, preferred_element_type=jnp.float32)
    for h in range(heads):
        block = mixed[h * rows : (h + 1) * rows] / totals[h]
        out_ref[:, h * width : (h + 1) * width] = block.astype(out_ref.dtype)


def attend(number, half, table, sink_bias, q, halo, near):
    heads, rows, width = q.shape[1:]
    rows = rows // 2
    tok_rows = halo.shape[2]
    vmem = pl.BlockSpec(memory_space=pltpu.VMEM)
    span = halo.shape[0] * tok_rows + near.shape[1]
    return pl.pallas_call(
        functools.partial(attend_kernel, tok_rows=tok_rows, number=number, half=half),
        out_shape=jax.ShapeDtypeStruct((rows, heads * width), jnp.bfloat16),
        in_specs=[vmem] * 5,
        out_specs=vmem,
        scratch_shapes=[
            pltpu.VMEM((heads * rows, span), jnp.float32),
            pltpu.VMEM((heads * rows, span), jnp.bfloat16),
        ],
        cost_estimate=pl.CostEstimate(
            flops=32 * heads * rows * span * width,
            bytes_accessed=halo.size * 2,
            transcendentals=heads * rows * span,
        ),
        compiler_params=pltpu.CompilerParams(vmem_limit_bytes=20 << 20),
        name="attend",
    )(table, sink_bias, q, halo, near)


def project_kernel(rows_ref, weight_ref, theirs_ref, *out_refs):
    per = out_refs[0].shape[0]
    step = 512

    for k in range(weight_ref.shape[1] // step):
        columns = slice(k * step, (k + 1) * step)
        total = jnp.dot(rows_ref[...], weight_ref[:, columns], preferred_element_type=jnp.float32)
        total = total.astype(jnp.bfloat16).astype(jnp.float32)
        total = total + theirs_ref[:, columns].astype(jnp.float32)
        for number, out_ref in enumerate(out_refs):
            out_ref[:, columns] = total[number * per : (number + 1) * per].astype(out_ref.dtype)


def project(rows, weight, theirs, members):
    vmem = pl.BlockSpec(memory_space=pltpu.VMEM)
    per, columns = rows.shape[0] // members, weight.shape[1]
    return pl.pallas_call(
        project_kernel,
        out_shape=[jax.ShapeDtypeStruct((per, columns), jnp.bfloat16)] * members,
        in_specs=[vmem] * 3,
        out_specs=[vmem] * members,
        cost_estimate=pl.CostEstimate(
            flops=2 * rows.size * columns, bytes_accessed=weight.size * 2, transcendentals=0
        ),
        compiler_params=pltpu.CompilerParams(vmem_limit_bytes=20 << 20),
        name="project",
    )(rows, weight, theirs)


def shards(queries, key_rows, value_rows, windows, sink_counts, sink_bias, out_weight):
    tok_rows, heads, width = queries.shape
    row_len = lax.axis_size("y")
    seq_len = lax.axis_size(SEQ)
    y, core = lax.axis_index("y"), lax.axis_index("core")
    first_pos = lax.axis_index(SEQ) * tok_rows
    stacked = jnp.stack([key_rows[:, 0], value_rows[:, 0]])
    before = lax.ppermute(stacked, SEQ, [(i, i + row_len) for i in range(seq_len - row_len)])
    def along_row():
        sinks = jnp.where(y == 0, stacked[:, :SINKS], 0)
        for axis, route in SPREAD[:3]:
            sinks = lax.optimization_barrier(sinks)
            sinks = sinks + lax.ppermute(sinks, axis, route)
        return sinks

    sinks = lax.cond(
        lax.axis_index(("zh", "x")) == 0,
        along_row,
        lambda: jnp.zeros((2, SINKS, width), stacked.dtype),
    )
    before, sinks = lax.optimization_barrier((before, sinks))
    sent = pack(y, stacked, before, row_len)
    halo = lax.all_to_all(sent, "y", 0, 0, axis_index_groups=[list(ORDER)], tiled=True)
    windows, sink_counts, sink_bias, _ = lax.optimization_barrier(
        (windows, sink_counts, sink_bias, sent)
    )
    for number, (axis, route) in enumerate(SPREAD[3:], 3):
        if number == len(SPREAD) - 1:
            sinks, queries = lax.optimization_barrier((sinks, queries))
        sinks = sinks + lax.ppermute(sinks, axis, route)
    near = jnp.concatenate(
        [stacked, jnp.pad(sinks, ((0, 0), (0, 64 - SINKS), (0, 0)))], axis=1
    )
    members, cores = lax.axis_size("zl"), lax.axis_size("core")
    own = tok_rows // (members * cores)
    member = lax.axis_index("zl")
    q = queries.reshape(2, 2, cores, own, heads, width)
    q = jnp.where(member % 2 == 1, jnp.stack([q[:, 1], q[:, 0]], axis=1), q)
    q = jnp.where(member // 2 == 1, jnp.stack([q[1], q[0]]), q)
    q = q.reshape(members, cores, own, heads, width)
    q = q.transpose(1, 3, 0, 2, 4).reshape(cores, heads, members * own, width)
    place = jnp.stack([first_pos, y, member, 1 - core, core]).astype(jnp.int32)
    table = jnp.concatenate([place, windows, sink_counts])
    table = jnp.pad(table, (0, -len(table) % 8))[:, None]
    bias = jnp.pad(sink_bias * width**0.5, (0, 8 - heads))[:, None]
    table = jnp.broadcast_to(table, (16, LANES))
    bias = jnp.broadcast_to(bias, (8, LANES))
    total = 0.0
    for half, distances in ((1, (3, 2)), (0, (1, 0))):
        theirs = attend(0, half, table, bias, q, halo, near)
        theirs = jnp.dot(theirs, out_weight, preferred_element_type=jnp.float32)
        theirs = theirs.astype(jnp.bfloat16)
        theirs = lax.ppermute(theirs, "core", [(0, 1), (1, 0)])
        mine = attend(1, half, table, bias, q, halo, near)
        parts = project(mine, out_weight, theirs, 2)
        for distance in distances:
            part = parts[distance % 2]
            if distance:
                route = [(i, i ^ distance) for i in range(members)]
                part = lax.ppermute(part, "zl", route)
            total += part.astype(jnp.float32)
    return total.astype(jnp.bfloat16)


def solution(mesh):
    split = Mesh(mesh.devices.reshape(2, 4, 8, 4, 2), SEQ + HEAD)
    return jax.shard_map(
        shards,
        mesh=split,
        in_specs=(
            P(SEQ, HEAD, None),
            P(SEQ, HEAD, None),
            P(SEQ, HEAD, None),
            P(HEAD),
            P(HEAD),
            P(HEAD),
            P(HEAD, None),
        ),
        out_specs=P(SEQ + HEAD, None),
        check_vma=False,
    )
```

```python
import functools

import jax
import jax.numpy as jnp
from jax import lax
from jax.experimental import pallas as pl
from jax.experimental.pallas import tpu as pltpu
from jax.sharding import Mesh
from jax.sharding import PartitionSpec as P

SINKS = 4
SEQ = ("zh", "x", "y")
HEAD = ("zl", "core")
LANES = 128
NEG = -1e30
LOG2E = 1.4426950408889634
SPREAD = (
    (SEQ, [(0, 1)]),
    (SEQ, [(0, 7), (1, 2)]),
    (SEQ, [(7, 5), (0, 6), (1, 3), (2, 4)]),
    (SEQ, [(i, i + 8) for i in range(8)]),
    (SEQ, [(i + j, i + k) for i in range(8) for j, k in ((0, 24), (8, 16))]),
    ("zh", [(0, 1)]),
)
ORDER = (4, 5, 6, 7, 3, 2, 1, 0)
ALWAYS, NEVER = 1 << 30, -(1 << 30)


def listed(number):
    return sum(jnp.where(number == k, y, 0) for k, y in enumerate(ORDER))


def pack_kernel(y_ref, own_ref, before_ref, sent_ref):
    target = listed(lax.broadcasted_iota(jnp.int32, y_ref.shape, 0))
    later = (target > y_ref[...]).astype(jnp.float32).astype(jnp.bfloat16)
    for number in range(sent_ref.shape[0]):
        chosen = later[number : number + 1]
        sent_ref[number] = own_ref[...] * chosen + before_ref[...] * (1 - chosen)


def pack(y, own, before, row_len):
    vmem = pl.BlockSpec(memory_space=pltpu.VMEM)
    return pl.pallas_call(
        pack_kernel,
        out_shape=jax.ShapeDtypeStruct((row_len, *own.shape), own.dtype),
        in_specs=[vmem] * 3,
        out_specs=vmem,
        compiler_params=pltpu.CompilerParams(vmem_limit_bytes=8 << 20),
        name="pack",
    )(jnp.full((row_len, LANES), y, jnp.int32), own, before)


def attend_kernel(
    table, bias, q_ref, halo_ref, near_ref, out_ref, score_ref, prob_ref, *, tok_rows, number
):
    heads, rows, width = q_ref.shape[1:]
    first_pos, y, member, part = (table[k : k + 1, :1] for k in (0, 1, 2, 3 + number))
    unit = LOG2E / width**0.5
    halo_len = halo_ref.shape[0] * tok_rows
    span = score_ref.shape[1]
    per = rows // 4
    row = lax.broadcasted_iota(jnp.int32, (rows, 1), 0)
    turn = sum((row >= per * k).astype(jnp.int32) for k in range(1, 4))
    query_pos = first_pos + (turn ^ member) * (2 * per) + part * per + row - turn * per
    place = lax.broadcasted_iota(jnp.int32, (1, halo_len), 1)
    block = sum((place >= k * tok_rows).astype(jnp.int32) for k in range(1, len(ORDER)))
    source = listed(block)
    halo_pos = first_pos + (source - y - block) * tok_rows + place
    halo_pos = halo_pos - jnp.where(source < y, 0, halo_len)
    near = lax.broadcasted_iota(jnp.int32, (1, span - halo_len), 1)
    is_sink = near >= tok_rows
    near_pos = jnp.where(is_sink, near - tok_rows, first_pos + near)
    first = (1 - part).astype(jnp.float32).astype(jnp.bfloat16)
    q = (q_ref[0] * first + q_ref[1] * (1 - first)).reshape(heads * rows, width)
    transposed = (((1,), (1,)), ((), ()))
    keys = jnp.concatenate([halo_ref[:, 0].reshape(halo_len, width), near_ref[0]], axis=0)
    score_ref[...] = lax.dot_general(q, keys, transposed, preferred_element_type=jnp.float32)
    totals = []
    for h in range(heads):
        window, count = (table[k : k + 1, :1] for k in (5 + h, 5 + heads + h))
        lowest = jnp.maximum(query_pos - window + 1, count)
        ranked = jnp.where(is_sink, jnp.where(near_pos < count, ALWAYS, NEVER), near_pos)
        mine = slice(h * rows, (h + 1) * rows)
        far = jnp.where(halo_pos >= lowest, score_ref[mine, :halo_len], NEG)
        close = score_ref[mine, halo_len:] + jnp.where(is_sink, bias[h : h + 1, :1], 0.0)
        close = jnp.where((near_pos <= query_pos) & (ranked >= lowest), close, NEG)
        top = jnp.maximum(
            jnp.max(far, axis=1, keepdims=True), jnp.max(close, axis=1, keepdims=True)
        )
        far = jnp.exp2((far - top) * unit)
        close = jnp.exp2((close - top) * unit)
        totals.append(jnp.sum(far, axis=1, keepdims=True) + jnp.sum(close, axis=1, keepdims=True))
        prob_ref[mine, :halo_len] = far.astype(jnp.bfloat16)
        prob_ref[mine, halo_len:] = close.astype(jnp.bfloat16)
    values = jnp.concatenate([halo_ref[:, 1].reshape(halo_len, width), near_ref[1]], axis=0)
    mixed = jnp.dot(prob_ref[...], values, preferred_element_type=jnp.float32)
    for h in range(heads):
        block = mixed[h * rows : (h + 1) * rows] / totals[h]
        out_ref[:, h * width : (h + 1) * width] = block.astype(out_ref.dtype)


def attend(number, table, sink_bias, q, halo, near):
    heads, rows, width = q.shape[1:]
    tok_rows = halo.shape[2]
    vmem = pl.BlockSpec(memory_space=pltpu.VMEM)
    span = halo.shape[0] * tok_rows + near.shape[1]
    return pl.pallas_call(
        functools.partial(attend_kernel, tok_rows=tok_rows, number=number),
        out_shape=jax.ShapeDtypeStruct((rows, heads * width), jnp.bfloat16),
        in_specs=[vmem] * 5,
        out_specs=vmem,
        scratch_shapes=[
            pltpu.VMEM((heads * rows, span), jnp.float32),
            pltpu.VMEM((heads * rows, span), jnp.bfloat16),
        ],
        cost_estimate=pl.CostEstimate(
            flops=32 * heads * rows * span * width,
            bytes_accessed=halo.size * 2,
            transcendentals=heads * rows * span,
        ),
        compiler_params=pltpu.CompilerParams(vmem_limit_bytes=20 << 20),
        name="attend",
    )(table, sink_bias, q, halo, near)


def project_kernel(rows_ref, weight_ref, theirs_ref, *out_refs):
    per = out_refs[0].shape[0]
    step = 512

    for k in range(weight_ref.shape[1] // step):
        columns = slice(k * step, (k + 1) * step)
        total = jnp.dot(rows_ref[...], weight_ref[:, columns], preferred_element_type=jnp.float32)
        total = total.astype(jnp.bfloat16).astype(jnp.float32)
        total = total + theirs_ref[:, columns].astype(jnp.float32)
        for number, out_ref in enumerate(out_refs):
            out_ref[:, columns] = total[number * per : (number + 1) * per].astype(out_ref.dtype)


def project(rows, weight, theirs, members):
    vmem = pl.BlockSpec(memory_space=pltpu.VMEM)
    per, columns = rows.shape[0] // members, weight.shape[1]
    return pl.pallas_call(
        project_kernel,
        out_shape=[jax.ShapeDtypeStruct((per, columns), jnp.bfloat16)] * members,
        in_specs=[vmem] * 3,
        out_specs=[vmem] * members,
        cost_estimate=pl.CostEstimate(
            flops=2 * rows.size * columns, bytes_accessed=weight.size * 2, transcendentals=0
        ),
        compiler_params=pltpu.CompilerParams(vmem_limit_bytes=20 << 20),
        name="project",
    )(rows, weight, theirs)


def shards(queries, key_rows, value_rows, windows, sink_counts, sink_bias, out_weight):
    tok_rows, heads, width = queries.shape
    row_len = lax.axis_size("y")
    seq_len = lax.axis_size(SEQ)
    y, core = lax.axis_index("y"), lax.axis_index("core")
    first_pos = lax.axis_index(SEQ) * tok_rows
    stacked = jnp.stack([key_rows[:, 0], value_rows[:, 0]])
    before = lax.ppermute(stacked, SEQ, [(i, i + row_len) for i in range(seq_len - row_len)])
    def along_row():
        sinks = jnp.where(y == 0, stacked[:, :SINKS], 0)
        for axis, route in SPREAD[:3]:
            sinks = lax.optimization_barrier(sinks)
            sinks = sinks + lax.ppermute(sinks, axis, route)
        return sinks

    sinks = lax.cond(
        lax.axis_index(("zh", "x")) == 0,
        along_row,
        lambda: jnp.zeros((2, SINKS, width), stacked.dtype),
    )
    before, sinks = lax.optimization_barrier((before, sinks))
    sent = pack(y, stacked, before, row_len)
    halo = lax.all_to_all(sent, "y", 0, 0, axis_index_groups=[list(ORDER)], tiled=True)
    windows, sink_counts, sink_bias, _ = lax.optimization_barrier(
        (windows, sink_counts, sink_bias, sent)
    )
    for number, (axis, route) in enumerate(SPREAD[3:], 3):
        if number == len(SPREAD) - 1:
            sinks, queries = lax.optimization_barrier((sinks, queries))
        sinks = sinks + lax.ppermute(sinks, axis, route)
    near = jnp.concatenate(
        [stacked, jnp.pad(sinks, ((0, 0), (0, 64 - SINKS), (0, 0)))], axis=1
    )
    members, cores = lax.axis_size("zl"), lax.axis_size("core")
    own = tok_rows // (members * cores)
    member = lax.axis_index("zl")
    q = queries.reshape(2, 2, cores, own, heads, width)
    q = jnp.where(member % 2 == 1, jnp.stack([q[:, 1], q[:, 0]], axis=1), q)
    q = jnp.where(member // 2 == 1, jnp.stack([q[1], q[0]]), q)
    q = q.reshape(members, cores, own, heads, width)
    q = q.transpose(1, 3, 0, 2, 4).reshape(cores, heads, members * own, width)
    place = jnp.stack([first_pos, y, member, 1 - core, core]).astype(jnp.int32)
    table = jnp.concatenate([place, windows, sink_counts])
    table = jnp.pad(table, (0, -len(table) % 8))[:, None]
    bias = jnp.pad(sink_bias * width**0.5, (0, 8 - heads))[:, None]
    table = jnp.broadcast_to(table, (16, LANES))
    bias = jnp.broadcast_to(bias, (8, LANES))
    theirs = attend(0, table, bias, q, halo, near)
    theirs = jnp.dot(theirs, out_weight, preferred_element_type=jnp.float32).astype(jnp.bfloat16)
    theirs = lax.ppermute(theirs, "core", [(0, 1), (1, 0)])
    mine = attend(1, table, bias, q, halo, near)
    parts = project(mine, out_weight, theirs, members)
    total = parts[0].astype(jnp.float32)
    for distance in (3, 1, 2):
        route = [(i, i ^ distance) for i in range(members)]
        total += lax.ppermute(parts[distance], "zl", route).astype(jnp.float32)
    return total.astype(jnp.bfloat16)


def solution(mesh):
    split = Mesh(mesh.devices.reshape(2, 4, 8, 4, 2), SEQ + HEAD)
    return jax.shard_map(
        shards,
        mesh=split,
        in_specs=(
            P(SEQ, HEAD, None),
            P(SEQ, HEAD, None),
            P(SEQ, HEAD, None),
            P(HEAD),
            P(HEAD),
            P(HEAD),
            P(HEAD, None),
        ),
        out_specs=P(SEQ + HEAD, None),
        check_vma=False,
    )
```

```python
import functools

import jax
import jax.numpy as jnp
from jax import lax
from jax.experimental import pallas as pl
from jax.experimental.pallas import tpu as pltpu
from jax.sharding import Mesh
from jax.sharding import PartitionSpec as P

SINKS = 4
SEQ = ("zh", "x", "y")
HEAD = ("zl", "core")
LANES = 128
NEG = -1e30
LOG2E = 1.4426950408889634
SPREAD = (
    (SEQ, [(0, 1)]),
    (SEQ, [(0, 7), (1, 2)]),
    (SEQ, [(7, 5), (0, 6), (1, 3), (2, 4)]),
    (SEQ, [(i, i + 8) for i in range(8)]),
    (SEQ, [(i + j, i + k) for i in range(8) for j, k in ((0, 24), (8, 16))]),
    ("zh", [(0, 1)]),
)
ORDER = (4, 5, 6, 7, 3, 2, 1, 0)
ALWAYS, NEVER = 1 << 30, -(1 << 30)


def listed(number):
    return sum(jnp.where(number == k, y, 0) for k, y in enumerate(ORDER))


def pack_kernel(y_ref, own_ref, before_ref, sent_ref):
    target = listed(lax.broadcasted_iota(jnp.int32, y_ref.shape, 0))
    later = (target > y_ref[...]).astype(jnp.float32).astype(jnp.bfloat16)
    for number in range(sent_ref.shape[0]):
        chosen = later[number : number + 1]
        sent_ref[number] = own_ref[...] * chosen + before_ref[...] * (1 - chosen)


def pack(y, own, before, row_len):
    vmem = pl.BlockSpec(memory_space=pltpu.VMEM)
    return pl.pallas_call(
        pack_kernel,
        out_shape=jax.ShapeDtypeStruct((row_len, *own.shape), own.dtype),
        in_specs=[vmem] * 3,
        out_specs=vmem,
        compiler_params=pltpu.CompilerParams(vmem_limit_bytes=8 << 20),
        name="pack",
    )(jnp.full((row_len, LANES), y, jnp.int32), own, before)


def attend_kernel(
    table, bias, q_ref, halo_ref, near_ref, out_ref, score_ref, prob_ref, *, tok_rows, number
):
    heads, rows, width = q_ref.shape[1:]
    first_pos, y, member, part = (table[k : k + 1, :1] for k in (0, 1, 2, 3 + number))
    unit = LOG2E / width**0.5
    halo_len = halo_ref.shape[0] * tok_rows
    span = score_ref.shape[1]
    per = rows // 4
    row = lax.broadcasted_iota(jnp.int32, (rows, 1), 0)
    turn = sum((row >= per * k).astype(jnp.int32) for k in range(1, 4))
    query_pos = first_pos + (turn ^ member) * (2 * per) + part * per + row - turn * per
    place = lax.broadcasted_iota(jnp.int32, (1, halo_len), 1)
    block = sum((place >= k * tok_rows).astype(jnp.int32) for k in range(1, len(ORDER)))
    source = listed(block)
    halo_pos = first_pos + (source - y - block) * tok_rows + place
    halo_pos = halo_pos - jnp.where(source < y, 0, halo_len)
    near = lax.broadcasted_iota(jnp.int32, (1, span - halo_len), 1)
    is_sink = near >= tok_rows
    near_pos = jnp.where(is_sink, near - tok_rows, first_pos + near)
    first = (1 - part).astype(jnp.float32).astype(jnp.bfloat16)
    q = (q_ref[0] * first + q_ref[1] * (1 - first)).reshape(heads * rows, width)
    transposed = (((1,), (1,)), ((), ()))
    keys = jnp.concatenate([halo_ref[:, 0].reshape(halo_len, width), near_ref[0]], axis=0)
    score_ref[...] = lax.dot_general(q, keys, transposed, preferred_element_type=jnp.float32)
    totals = []
    for h in range(heads):
        window, count = (table[k : k + 1, :1] for k in (5 + h, 5 + heads + h))
        lowest = jnp.maximum(query_pos - window + 1, count)
        ranked = jnp.where(is_sink, jnp.where(near_pos < count, ALWAYS, NEVER), near_pos)
        mine = slice(h * rows, (h + 1) * rows)
        far = jnp.where(halo_pos >= lowest, score_ref[mine, :halo_len], NEG)
        close = score_ref[mine, halo_len:] + jnp.where(is_sink, bias[h : h + 1, :1], 0.0)
        close = jnp.where((near_pos <= query_pos) & (ranked >= lowest), close, NEG)
        top = jnp.maximum(
            jnp.max(far, axis=1, keepdims=True), jnp.max(close, axis=1, keepdims=True)
        )
        far = jnp.exp2((far - top) * unit)
        close = jnp.exp2((close - top) * unit)
        totals.append(jnp.sum(far, axis=1, keepdims=True) + jnp.sum(close, axis=1, keepdims=True))
        prob_ref[mine, :halo_len] = far.astype(jnp.bfloat16)
        prob_ref[mine, halo_len:] = close.astype(jnp.bfloat16)
    values = jnp.concatenate([halo_ref[:, 1].reshape(halo_len, width), near_ref[1]], axis=0)
    mixed = jnp.dot(prob_ref[...], values, preferred_element_type=jnp.float32)
    for h in range(heads):
        block = mixed[h * rows : (h + 1) * rows] / totals[h]
        out_ref[:, h * width : (h + 1) * width] = block.astype(out_ref.dtype)


def attend(number, table, sink_bias, q, halo, near):
    heads, rows, width = q.shape[1:]
    tok_rows = halo.shape[2]
    vmem = pl.BlockSpec(memory_space=pltpu.VMEM)
    span = halo.shape[0] * tok_rows + near.shape[1]
    return pl.pallas_call(
        functools.partial(attend_kernel, tok_rows=tok_rows, number=number),
        out_shape=jax.ShapeDtypeStruct((rows, heads * width), jnp.bfloat16),
        in_specs=[vmem] * 5,
        out_specs=vmem,
        scratch_shapes=[
            pltpu.VMEM((heads * rows, span), jnp.float32),
            pltpu.VMEM((heads * rows, span), jnp.bfloat16),
        ],
        cost_estimate=pl.CostEstimate(
            flops=32 * heads * rows * span * width,
            bytes_accessed=halo.size * 2,
            transcendentals=heads * rows * span,
        ),
        compiler_params=pltpu.CompilerParams(vmem_limit_bytes=20 << 20),
        name="attend",
    )(table, sink_bias, q, halo, near)


def project_kernel(rows_ref, weight_ref, theirs_ref, *out_refs):
    per = out_refs[0].shape[0]
    step = 512

    for k in range(weight_ref.shape[1] // step):
        columns = slice(k * step, (k + 1) * step)
        total = jnp.dot(rows_ref[...], weight_ref[:, columns], preferred_element_type=jnp.float32)
        total = total.astype(jnp.bfloat16).astype(jnp.float32)
        total = total + theirs_ref[:, columns].astype(jnp.float32)
        for number, out_ref in enumerate(out_refs):
            out_ref[:, columns] = total[number * per : (number + 1) * per].astype(out_ref.dtype)


def project(rows, weight, theirs, members):
    vmem = pl.BlockSpec(memory_space=pltpu.VMEM)
    per, columns = rows.shape[0] // members, weight.shape[1]
    return pl.pallas_call(
        project_kernel,
        out_shape=[jax.ShapeDtypeStruct((per, columns), jnp.bfloat16)] * members,
        in_specs=[vmem] * 3,
        out_specs=[vmem] * members,
        cost_estimate=pl.CostEstimate(
            flops=2 * rows.size * columns, bytes_accessed=weight.size * 2, transcendentals=0
        ),
        compiler_params=pltpu.CompilerParams(vmem_limit_bytes=20 << 20),
        name="project",
    )(rows, weight, theirs)


def shards(queries, key_rows, value_rows, windows, sink_counts, sink_bias, out_weight):
    tok_rows, heads, width = queries.shape
    row_len = lax.axis_size("y")
    seq_len = lax.axis_size(SEQ)
    y, core = lax.axis_index("y"), lax.axis_index("core")
    first_pos = lax.axis_index(SEQ) * tok_rows
    stacked = jnp.stack([key_rows[:, 0], value_rows[:, 0]])
    first_row = lax.axis_index(("zh", "x")) == 0

    def along_row(steps, sinks):
        for axis, route in steps:
            sinks = lax.optimization_barrier(sinks)
            sinks = sinks + lax.ppermute(sinks, axis, route)
        return sinks

    sinks = lax.cond(
        first_row,
        lambda: along_row(SPREAD[:1], jnp.where(y == 0, stacked[:, :SINKS], 0)),
        lambda: jnp.zeros((2, SINKS, width), stacked.dtype),
    )
    stacked, sinks = lax.optimization_barrier((stacked, sinks))
    before = lax.ppermute(stacked, SEQ, [(i, i + row_len) for i in range(seq_len - row_len)])
    sinks = lax.cond(
        first_row, lambda v: along_row(SPREAD[1:3], v), lambda v: v, sinks
    )
    before, sinks = lax.optimization_barrier((before, sinks))
    sent = pack(y, stacked, before, row_len)
    halo = lax.all_to_all(sent, "y", 0, 0, axis_index_groups=[list(ORDER)], tiled=True)
    windows, sink_counts, sink_bias, _ = lax.optimization_barrier(
        (windows, sink_counts, sink_bias, sent)
    )
    for number, (axis, route) in enumerate(SPREAD[3:], 3):
        if number == len(SPREAD) - 1:
            sinks, queries = lax.optimization_barrier((sinks, queries))
        sinks = sinks + lax.ppermute(sinks, axis, route)
    near = jnp.concatenate(
        [stacked, jnp.pad(sinks, ((0, 0), (0, 64 - SINKS), (0, 0)))], axis=1
    )
    members, cores = lax.axis_size("zl"), lax.axis_size("core")
    own = tok_rows // (members * cores)
    member = lax.axis_index("zl")
    q = queries.reshape(2, 2, cores, own, heads, width)
    q = jnp.where(member % 2 == 1, jnp.stack([q[:, 1], q[:, 0]], axis=1), q)
    q = jnp.where(member // 2 == 1, jnp.stack([q[1], q[0]]), q)
    q = q.reshape(members, cores, own, heads, width)
    q = q.transpose(1, 3, 0, 2, 4).reshape(cores, heads, members * own, width)
    place = jnp.stack([first_pos, y, member, 1 - core, core]).astype(jnp.int32)
    table = jnp.concatenate([place, windows, sink_counts])
    table = jnp.pad(table, (0, -len(table) % 8))[:, None]
    bias = jnp.pad(sink_bias * width**0.5, (0, 8 - heads))[:, None]
    table = jnp.broadcast_to(table, (16, LANES))
    bias = jnp.broadcast_to(bias, (8, LANES))
    theirs = attend(0, table, bias, q, halo, near)
    theirs = jnp.dot(theirs, out_weight, preferred_element_type=jnp.float32).astype(jnp.bfloat16)
    theirs = lax.ppermute(theirs, "core", [(0, 1), (1, 0)])
    mine = attend(1, table, bias, q, halo, near)
    parts = project(mine, out_weight, theirs, members)
    total = parts[0].astype(jnp.float32)
    for distance in (3, 1, 2):
        route = [(i, i ^ distance) for i in range(members)]
        total += lax.ppermute(parts[distance], "zl", route).astype(jnp.float32)
    return total.astype(jnp.bfloat16)


def solution(mesh):
    split = Mesh(mesh.devices.reshape(2, 4, 8, 4, 2), SEQ + HEAD)
    return jax.shard_map(
        shards,
        mesh=split,
        in_specs=(
            P(SEQ, HEAD, None),
            P(SEQ, HEAD, None),
            P(SEQ, HEAD, None),
            P(HEAD),
            P(HEAD),
            P(HEAD),
            P(HEAD, None),
        ),
        out_specs=P(SEQ + HEAD, None),
        check_vma=False,
    )
```

```python
import functools

import jax
import jax.numpy as jnp
from jax import lax
from jax.experimental import pallas as pl
from jax.experimental.pallas import tpu as pltpu
from jax.sharding import Mesh
from jax.sharding import PartitionSpec as P

SINKS = 4
SEQ = ("zh", "x", "y")
HEAD = ("zl", "core")
LANES = 128
NEG = -1e30
LOG2E = 1.4426950408889634
SPREAD = (
    (SEQ, [(0, 1)]),
    (SEQ, [(0, 7), (1, 2)]),
    (SEQ, [(7, 5), (0, 6), (1, 3), (2, 4)]),
    (SEQ, [(i, i + 8) for i in range(8)]),
    (SEQ, [(i + j, i + k) for i in range(8) for j, k in ((0, 24), (8, 16))]),
    ("zh", [(0, 1)]),
)
ORDER = (4, 5, 6, 7, 3, 2, 1, 0)
ALWAYS, NEVER = 1 << 30, -(1 << 30)


def listed(number):
    return sum(jnp.where(number == k, y, 0) for k, y in enumerate(ORDER))


def pack_kernel(own_ref, before_ref, sent_ref, done):
    y = lax.axis_index("y")
    for number, target in enumerate(ORDER):

        @pl.when(target > y)
        def _():
            pltpu.make_async_copy(own_ref, sent_ref.at[number], done.at[number]).start()

        @pl.when(target <= y)
        def _():
            pltpu.make_async_copy(before_ref, sent_ref.at[number], done.at[number]).start()

    for number in range(len(ORDER)):
        pltpu.make_async_copy(own_ref, sent_ref.at[number], done.at[number]).wait()


def pack(own, before, row_len):
    vmem = pl.BlockSpec(memory_space=pltpu.VMEM)
    return pl.pallas_call(
        pack_kernel,
        out_shape=jax.ShapeDtypeStruct((row_len, *own.shape), own.dtype),
        in_specs=[vmem] * 2,
        out_specs=pl.BlockSpec(memory_space=pl.ANY),
        scratch_shapes=[pltpu.SemaphoreType.DMA((row_len,))],
        compiler_params=pltpu.CompilerParams(vmem_limit_bytes=8 << 20),
        name="pack",
    )(own, before)


def attend_kernel(
    table, bias, q_ref, halo_ref, near_ref, out_ref, score_ref, prob_ref, *, tok_rows, number
):
    heads, rows, width = q_ref.shape[1:]
    first_pos, y, member, part = (table[k : k + 1, :1] for k in (0, 1, 2, 3 + number))
    unit = LOG2E / width**0.5
    halo_len = halo_ref.shape[0] * tok_rows
    span = score_ref.shape[1]
    per = rows // 4
    row = lax.broadcasted_iota(jnp.int32, (rows, 1), 0)
    turn = sum((row >= per * k).astype(jnp.int32) for k in range(1, 4))
    query_pos = first_pos + (turn ^ member) * (2 * per) + part * per + row - turn * per
    place = lax.broadcasted_iota(jnp.int32, (1, halo_len), 1)
    block = sum((place >= k * tok_rows).astype(jnp.int32) for k in range(1, len(ORDER)))
    source = listed(block)
    halo_pos = first_pos + (source - y - block) * tok_rows + place
    halo_pos = halo_pos - jnp.where(source < y, 0, halo_len)
    near = lax.broadcasted_iota(jnp.int32, (1, span - halo_len), 1)
    is_sink = near >= tok_rows
    near_pos = jnp.where(is_sink, near - tok_rows, first_pos + near)
    first = (1 - part).astype(jnp.float32).astype(jnp.bfloat16)
    q = (q_ref[0] * first + q_ref[1] * (1 - first)).reshape(heads * rows, width)
    transposed = (((1,), (1,)), ((), ()))
    keys = jnp.concatenate([halo_ref[:, 0].reshape(halo_len, width), near_ref[0]], axis=0)
    values = jnp.concatenate([halo_ref[:, 1].reshape(halo_len, width), near_ref[1]], axis=0)
    for pair in range(0, heads, 2):
        both = slice(pair * rows, (pair + 2) * rows)
        score_ref[both] = lax.dot_general(
            q[both], keys, transposed, preferred_element_type=jnp.float32
        )
        totals = []
        for h in range(pair, pair + 2):
            window, count = (table[k : k + 1, :1] for k in (5 + h, 5 + heads + h))
            lowest = jnp.maximum(query_pos - window + 1, count)
            ranked = jnp.where(is_sink, jnp.where(near_pos < count, ALWAYS, NEVER), near_pos)
            mine = slice(h * rows, (h + 1) * rows)
            far = jnp.where(halo_pos >= lowest, score_ref[mine, :halo_len], NEG)
            close = score_ref[mine, halo_len:] + jnp.where(is_sink, bias[h : h + 1, :1], 0.0)
            close = jnp.where((near_pos <= query_pos) & (ranked >= lowest), close, NEG)
            top = jnp.maximum(
                jnp.max(far, axis=1, keepdims=True), jnp.max(close, axis=1, keepdims=True)
            )
            far = jnp.exp2((far - top) * unit)
            close = jnp.exp2((close - top) * unit)
            totals.append(
                jnp.sum(far, axis=1, keepdims=True) + jnp.sum(close, axis=1, keepdims=True)
            )
            prob_ref[mine, :halo_len] = far.astype(jnp.bfloat16)
            prob_ref[mine, halo_len:] = close.astype(jnp.bfloat16)
        mixed = jnp.dot(prob_ref[both], values, preferred_element_type=jnp.float32)
        for h in range(2):
            block = mixed[h * rows : (h + 1) * rows] / totals[h]
            first_lane = (pair + h) * width
            out_ref[:, first_lane : first_lane + width] = block.astype(out_ref.dtype)


def attend(number, table, sink_bias, q, halo, near):
    heads, rows, width = q.shape[1:]
    tok_rows = halo.shape[2]
    vmem = pl.BlockSpec(memory_space=pltpu.VMEM)
    span = halo.shape[0] * tok_rows + near.shape[1]
    return pl.pallas_call(
        functools.partial(attend_kernel, tok_rows=tok_rows, number=number),
        out_shape=jax.ShapeDtypeStruct((rows, heads * width), jnp.bfloat16),
        in_specs=[vmem] * 5,
        out_specs=vmem,
        scratch_shapes=[
            pltpu.VMEM((heads * rows, span), jnp.float32),
            pltpu.VMEM((heads * rows, span), jnp.bfloat16),
        ],
        cost_estimate=pl.CostEstimate(
            flops=32 * heads * rows * span * width,
            bytes_accessed=halo.size * 2,
            transcendentals=heads * rows * span,
        ),
        compiler_params=pltpu.CompilerParams(vmem_limit_bytes=20 << 20),
        name="attend",
    )(table, sink_bias, q, halo, near)


def project_kernel(rows_ref, weight_ref, theirs_ref, *out_refs):
    per = out_refs[0].shape[0]
    step = 512

    for k in range(weight_ref.shape[1] // step):
        columns = slice(k * step, (k + 1) * step)
        total = jnp.dot(rows_ref[...], weight_ref[:, columns], preferred_element_type=jnp.float32)
        total = total.astype(jnp.bfloat16).astype(jnp.float32)
        total = total + theirs_ref[:, columns].astype(jnp.float32)
        for number, out_ref in enumerate(out_refs):
            out_ref[:, columns] = total[number * per : (number + 1) * per].astype(out_ref.dtype)


def project(rows, weight, theirs, members):
    vmem = pl.BlockSpec(memory_space=pltpu.VMEM)
    per, columns = rows.shape[0] // members, weight.shape[1]
    return pl.pallas_call(
        project_kernel,
        out_shape=[jax.ShapeDtypeStruct((per, columns), jnp.bfloat16)] * members,
        in_specs=[vmem] * 3,
        out_specs=[vmem] * members,
        cost_estimate=pl.CostEstimate(
            flops=2 * rows.size * columns, bytes_accessed=weight.size * 2, transcendentals=0
        ),
        compiler_params=pltpu.CompilerParams(vmem_limit_bytes=20 << 20),
        name="project",
    )(rows, weight, theirs)


def shards(queries, key_rows, value_rows, windows, sink_counts, sink_bias, out_weight):
    tok_rows, heads, width = queries.shape
    row_len = lax.axis_size("y")
    seq_len = lax.axis_size(SEQ)
    y, core = lax.axis_index("y"), lax.axis_index("core")
    first_pos = lax.axis_index(SEQ) * tok_rows
    stacked = jnp.stack([key_rows[:, 0], value_rows[:, 0]])
    first_row = lax.axis_index(("zh", "x")) == 0

    def along_row(steps, sinks):
        for axis, route in steps:
            sinks = lax.optimization_barrier(sinks)
            sinks = sinks + lax.ppermute(sinks, axis, route)
        return sinks

    sinks = lax.cond(
        first_row,
        lambda: along_row(SPREAD[:1], jnp.where(y == 0, stacked[:, :SINKS], 0)),
        lambda: jnp.zeros((2, SINKS, width), stacked.dtype),
    )
    stacked, sinks = lax.optimization_barrier((stacked, sinks))
    before = lax.ppermute(stacked, SEQ, [(i, i + row_len) for i in range(seq_len - row_len)])
    sinks = lax.cond(
        first_row, lambda v: along_row(SPREAD[1:3], v), lambda v: v, sinks
    )
    before, sinks = lax.optimization_barrier((before, sinks))
    sent = pack(stacked, before, row_len)
    halo = lax.all_to_all(sent, "y", 0, 0, axis_index_groups=[list(ORDER)], tiled=True)
    windows, sink_counts, sink_bias, _ = lax.optimization_barrier(
        (windows, sink_counts, sink_bias, sent)
    )
    for number, (axis, route) in enumerate(SPREAD[3:], 3):
        if number == len(SPREAD) - 1:
            sinks, queries = lax.optimization_barrier((sinks, queries))
        sinks = sinks + lax.ppermute(sinks, axis, route)
    near = jnp.concatenate(
        [stacked, jnp.pad(sinks, ((0, 0), (0, 64 - SINKS), (0, 0)))], axis=1
    )
    members, cores = lax.axis_size("zl"), lax.axis_size("core")
    own = tok_rows // (members * cores)
    member = lax.axis_index("zl")
    q = queries.reshape(2, 2, cores, own, heads, width)
    q = jnp.where(member % 2 == 1, jnp.stack([q[:, 1], q[:, 0]], axis=1), q)
    q = jnp.where(member // 2 == 1, jnp.stack([q[1], q[0]]), q)
    q = q.reshape(members, cores, own, heads, width)
    q = q.transpose(1, 3, 0, 2, 4).reshape(cores, heads, members * own, width)
    place = jnp.stack([first_pos, y, member, 1 - core, core]).astype(jnp.int32)
    table = jnp.concatenate([place, windows, sink_counts])
    table = jnp.pad(table, (0, -len(table) % 8))[:, None]
    bias = jnp.pad(sink_bias * width**0.5, (0, 8 - heads))[:, None]
    table = jnp.broadcast_to(table, (16, LANES))
    bias = jnp.broadcast_to(bias, (8, LANES))
    theirs = attend(0, table, bias, q, halo, near)
    theirs = jnp.dot(theirs, out_weight, preferred_element_type=jnp.float32).astype(jnp.bfloat16)
    theirs = lax.ppermute(theirs, "core", [(0, 1), (1, 0)])
    mine = attend(1, table, bias, q, halo, near)
    parts = project(mine, out_weight, theirs, members)
    total = parts[0].astype(jnp.float32)
    for distance in (3, 1, 2):
        route = [(i, i ^ distance) for i in range(members)]
        total += lax.ppermute(parts[distance], "zl", route).astype(jnp.float32)
    return total.astype(jnp.bfloat16)


def solution(mesh):
    split = Mesh(mesh.devices.reshape(2, 4, 8, 4, 2), SEQ + HEAD)
    return jax.shard_map(
        shards,
        mesh=split,
        in_specs=(
            P(SEQ, HEAD, None),
            P(SEQ, HEAD, None),
            P(SEQ, HEAD, None),
            P(HEAD),
            P(HEAD),
            P(HEAD),
            P(HEAD, None),
        ),
        out_specs=P(SEQ + HEAD, None),
        check_vma=False,
    )
```

```python
import functools

import jax
import jax.numpy as jnp
from jax import lax
from jax.experimental import pallas as pl
from jax.experimental.pallas import tpu as pltpu
from jax.sharding import Mesh
from jax.sharding import PartitionSpec as P

SINKS = 4
SEQ = ("zh", "x", "y")
HEAD = ("zl", "core")
LANES = 128
NEG = -1e30
LOG2E = 1.4426950408889634
SPREAD = (
    (SEQ, [(0, 1)]),
    (SEQ, [(0, 7), (1, 2)]),
    (SEQ, [(7, 5), (0, 6), (1, 3), (2, 4)]),
    (SEQ, [(i, i + 8) for i in range(8)]),
    (SEQ, [(i + j, i + k) for i in range(8) for j, k in ((0, 24), (8, 16))]),
    ("zh", [(0, 1)]),
)
ORDER = (5, 4, 3, 2, 6, 7, 0, 1)
ALWAYS, NEVER = 1 << 30, -(1 << 30)


def listed(number):
    return sum(jnp.where(number == k, y, 0) for k, y in enumerate(ORDER))


def pack_kernel(own_ref, before_ref, sent_ref, done):
    y = lax.axis_index("y")
    for number, target in enumerate(ORDER):

        @pl.when(target > y)
        def _():
            pltpu.make_async_copy(own_ref, sent_ref.at[number], done.at[number]).start()

        @pl.when(target <= y)
        def _():
            pltpu.make_async_copy(before_ref, sent_ref.at[number], done.at[number]).start()

    for number in range(len(ORDER)):
        pltpu.make_async_copy(own_ref, sent_ref.at[number], done.at[number]).wait()


def pack(own, before, row_len):
    vmem = pl.BlockSpec(memory_space=pltpu.VMEM)
    return pl.pallas_call(
        pack_kernel,
        out_shape=jax.ShapeDtypeStruct((row_len, *own.shape), own.dtype),
        in_specs=[vmem] * 2,
        out_specs=pl.BlockSpec(memory_space=pl.ANY),
        scratch_shapes=[pltpu.SemaphoreType.DMA((row_len,))],
        compiler_params=pltpu.CompilerParams(vmem_limit_bytes=8 << 20),
        name="pack",
    )(own, before)


def attend_kernel(
    table, bias, q_ref, halo_ref, near_ref, out_ref, score_ref, prob_ref, *, tok_rows, number
):
    heads, rows, width = q_ref.shape[1:]
    first_pos, y, member, part = (table[k : k + 1, :1] for k in (0, 1, 2, 3 + number))
    unit = LOG2E / width**0.5
    halo_len = halo_ref.shape[0] * tok_rows
    span = score_ref.shape[1]
    per = rows // 4
    row = lax.broadcasted_iota(jnp.int32, (rows, 1), 0)
    turn = sum((row >= per * k).astype(jnp.int32) for k in range(1, 4))
    query_pos = first_pos + (turn ^ member) * (2 * per) + part * per + row - turn * per
    place = lax.broadcasted_iota(jnp.int32, (1, halo_len), 1)
    block = sum((place >= k * tok_rows).astype(jnp.int32) for k in range(1, len(ORDER)))
    source = listed(block)
    halo_pos = first_pos + (source - y - block) * tok_rows + place
    halo_pos = halo_pos - jnp.where(source < y, 0, halo_len)
    near = lax.broadcasted_iota(jnp.int32, (1, span - halo_len), 1)
    is_sink = near >= tok_rows
    near_pos = jnp.where(is_sink, near - tok_rows, first_pos + near)
    first = (1 - part).astype(jnp.float32).astype(jnp.bfloat16)
    q = (q_ref[0] * first + q_ref[1] * (1 - first)).reshape(heads * rows, width)
    transposed = (((1,), (1,)), ((), ()))
    keys = jnp.concatenate([halo_ref[:, 0].reshape(halo_len, width), near_ref[0]], axis=0)
    values = jnp.concatenate([halo_ref[:, 1].reshape(halo_len, width), near_ref[1]], axis=0)
    for pair in range(0, heads, 2):
        both = slice(pair * rows, (pair + 2) * rows)
        score_ref[both] = lax.dot_general(
            q[both], keys, transposed, preferred_element_type=jnp.float32
        )
        totals = []
        for h in range(pair, pair + 2):
            window, count = (table[k : k + 1, :1] for k in (5 + h, 5 + heads + h))
            lowest = jnp.maximum(query_pos - window + 1, count)
            ranked = jnp.where(is_sink, jnp.where(near_pos < count, ALWAYS, NEVER), near_pos)
            mine = slice(h * rows, (h + 1) * rows)
            far = jnp.where(halo_pos >= lowest, score_ref[mine, :halo_len], NEG)
            close = score_ref[mine, halo_len:] + jnp.where(is_sink, bias[h : h + 1, :1], 0.0)
            close = jnp.where((near_pos <= query_pos) & (ranked >= lowest), close, NEG)
            top = jnp.maximum(
                jnp.max(far, axis=1, keepdims=True), jnp.max(close, axis=1, keepdims=True)
            )
            far = jnp.exp2((far - top) * unit)
            close = jnp.exp2((close - top) * unit)
            totals.append(
                jnp.sum(far, axis=1, keepdims=True) + jnp.sum(close, axis=1, keepdims=True)
            )
            prob_ref[mine, :halo_len] = far.astype(jnp.bfloat16)
            prob_ref[mine, halo_len:] = close.astype(jnp.bfloat16)
        mixed = jnp.dot(prob_ref[both], values, preferred_element_type=jnp.float32)
        for h in range(2):
            block = mixed[h * rows : (h + 1) * rows] / totals[h]
            first_lane = (pair + h) * width
            out_ref[:, first_lane : first_lane + width] = block.astype(out_ref.dtype)


def attend(number, table, sink_bias, q, halo, near):
    heads, rows, width = q.shape[1:]
    tok_rows = halo.shape[2]
    vmem = pl.BlockSpec(memory_space=pltpu.VMEM)
    span = halo.shape[0] * tok_rows + near.shape[1]
    return pl.pallas_call(
        functools.partial(attend_kernel, tok_rows=tok_rows, number=number),
        out_shape=jax.ShapeDtypeStruct((rows, heads * width), jnp.bfloat16),
        in_specs=[vmem] * 5,
        out_specs=vmem,
        scratch_shapes=[
            pltpu.VMEM((heads * rows, span), jnp.float32),
            pltpu.VMEM((heads * rows, span), jnp.bfloat16),
        ],
        cost_estimate=pl.CostEstimate(
            flops=32 * heads * rows * span * width,
            bytes_accessed=halo.size * 2,
            transcendentals=heads * rows * span,
        ),
        compiler_params=pltpu.CompilerParams(vmem_limit_bytes=20 << 20),
        name="attend",
    )(table, sink_bias, q, halo, near)


def project_kernel(rows_ref, weight_ref, theirs_ref, *out_refs):
    per = out_refs[0].shape[0]
    step = 512

    for k in range(weight_ref.shape[1] // step):
        columns = slice(k * step, (k + 1) * step)
        total = jnp.dot(rows_ref[...], weight_ref[:, columns], preferred_element_type=jnp.float32)
        total = total.astype(jnp.bfloat16).astype(jnp.float32)
        total = total + theirs_ref[:, columns].astype(jnp.float32)
        for number, out_ref in enumerate(out_refs):
            out_ref[:, columns] = total[number * per : (number + 1) * per].astype(out_ref.dtype)


def project(rows, weight, theirs, members):
    vmem = pl.BlockSpec(memory_space=pltpu.VMEM)
    per, columns = rows.shape[0] // members, weight.shape[1]
    return pl.pallas_call(
        project_kernel,
        out_shape=[jax.ShapeDtypeStruct((per, columns), jnp.bfloat16)] * members,
        in_specs=[vmem] * 3,
        out_specs=[vmem] * members,
        cost_estimate=pl.CostEstimate(
            flops=2 * rows.size * columns, bytes_accessed=weight.size * 2, transcendentals=0
        ),
        compiler_params=pltpu.CompilerParams(vmem_limit_bytes=20 << 20),
        name="project",
    )(rows, weight, theirs)


def shards(queries, key_rows, value_rows, windows, sink_counts, sink_bias, out_weight):
    tok_rows, heads, width = queries.shape
    row_len = lax.axis_size("y")
    seq_len = lax.axis_size(SEQ)
    y, core = lax.axis_index("y"), lax.axis_index("core")
    first_pos = lax.axis_index(SEQ) * tok_rows
    stacked = jnp.stack([key_rows[:, 0], value_rows[:, 0]])
    first_row = lax.axis_index(("zh", "x")) == 0

    def along_row(steps, sinks):
        for axis, route in steps:
            sinks = lax.optimization_barrier(sinks)
            sinks = sinks + lax.ppermute(sinks, axis, route)
        return sinks

    sinks = lax.cond(
        first_row,
        lambda: along_row(SPREAD[:1], jnp.where(y == 0, stacked[:, :SINKS], 0)),
        lambda: jnp.zeros((2, SINKS, width), stacked.dtype),
    )
    stacked, sinks = lax.optimization_barrier((stacked, sinks))
    before = lax.ppermute(stacked, SEQ, [(i, i + row_len) for i in range(seq_len - row_len)])
    sinks = lax.cond(
        first_row, lambda v: along_row(SPREAD[1:3], v), lambda v: v, sinks
    )
    before, sinks = lax.optimization_barrier((before, sinks))
    sent = pack(stacked, before, row_len)
    halo = lax.all_to_all(sent, "y", 0, 0, axis_index_groups=[list(ORDER)], tiled=True)
    windows, sink_counts, sink_bias, _ = lax.optimization_barrier(
        (windows, sink_counts, sink_bias, sent)
    )
    for number, (axis, route) in enumerate(SPREAD[3:], 3):
        if number == len(SPREAD) - 2:
            sinks, queries = lax.optimization_barrier((sinks, queries))
        sinks = sinks + lax.ppermute(sinks, axis, route)
    near = jnp.concatenate(
        [stacked, jnp.pad(sinks, ((0, 0), (0, 64 - SINKS), (0, 0)))], axis=1
    )
    members, cores = lax.axis_size("zl"), lax.axis_size("core")
    own = tok_rows // (members * cores)
    member = lax.axis_index("zl")
    q = queries.reshape(2, 2, cores, own, heads, width)
    q = jnp.where(member % 2 == 1, jnp.stack([q[:, 1], q[:, 0]], axis=1), q)
    q = jnp.where(member // 2 == 1, jnp.stack([q[1], q[0]]), q)
    q = q.reshape(members, cores, own, heads, width)
    q = q.transpose(1, 3, 0, 2, 4).reshape(cores, heads, members * own, width)
    place = jnp.stack([first_pos, y, member, 1 - core, core]).astype(jnp.int32)
    table = jnp.concatenate([place, windows, sink_counts])
    table = jnp.pad(table, (0, -len(table) % 8))[:, None]
    bias = jnp.pad(sink_bias * width**0.5, (0, 8 - heads))[:, None]
    table = jnp.broadcast_to(table, (16, LANES))
    bias = jnp.broadcast_to(bias, (8, LANES))
    theirs = attend(0, table, bias, q, halo, near)
    theirs = jnp.dot(theirs, out_weight, preferred_element_type=jnp.float32).astype(jnp.bfloat16)
    theirs = lax.ppermute(theirs, "core", [(0, 1), (1, 0)])
    mine = attend(1, table, bias, q, halo, near)
    parts = project(mine, out_weight, theirs, members)
    total = parts[0].astype(jnp.float32)
    for distance in (2, 1, 3):
        route = [(i, i ^ distance) for i in range(members)]
        total += lax.ppermute(parts[distance], "zl", route).astype(jnp.float32)
    return total.astype(jnp.bfloat16)


def solution(mesh):
    split = Mesh(mesh.devices.reshape(2, 4, 8, 4, 2), SEQ + HEAD)
    return jax.shard_map(
        shards,
        mesh=split,
        in_specs=(
            P(SEQ, HEAD, None),
            P(SEQ, HEAD, None),
            P(SEQ, HEAD, None),
            P(HEAD),
            P(HEAD),
            P(HEAD),
            P(HEAD, None),
        ),
        out_specs=P(SEQ + HEAD, None),
        check_vma=False,
    )
```
